32 devices in a mesh: curve: 8 (over z, y), seg: 4 (over x, core).
Axes of the slice: x: 2, y: 2, z: 4, core: 2. Of those that a mesh axis runs over, the one named last changes fastest.
Arguments:
- solution: bfloat16 [16384, 128], P(('curve', 'seg')), may hold values from -6 to 6
- viscosity: float32 [131072], P(('curve', 'seg')), may hold values from 0.1 to 10
- slot_index: int32 [131072, 4], P(('curve', 'seg')), may hold values from 0 to 1279, as said below
- slot_weight: int32 [131072, 4], P(('curve', 'seg')), may hold values from -1 to 8, as said below
- mirror_rows: int32 [32, 4, 192], P(('curve', 'seg')), may hold values from 0 to 511
- ghost_live: int32 [32, 4], P(('curve', 'seg')), may hold values from 0 to 192, as said below
- cell_count: int32 [32], P(('curve', 'seg')), may hold values from 512 to 4096, as said below
- viscous_block: bfloat16 [128, 128], replicated, may hold values from -0.5 to 0.5
- pressure_block: bfloat16 [128, 128], replicated, may hold values from -0.5 to 0.5
Outputs:
- residual: float32 [16384, 128], P(('curve', 'seg'))
The draws below stay inside these ranges and needn't reach their ends.
Inputs may be any that keep to these rules, and one draw needn't show every extreme that they name: `slot_index`: column 0 of each element is one of its device's owned blocks; other columns point to owned blocks or to ghost entries; ghost entries past a list's live count read zeros. `slot_weight`: each entry is one of -1, 3, 6, 8; column 0 is 8. `ghost_live`: some list is full in every draw. `cell_count`: some device is full in every draw; loads are skewed.
All inputs are finite; a program needn't handle non-finite values.
Results may differ from the reference program's by a relative error of at most 0.0035.
Values may be sent and summed in bfloat16 or wider, within the bound.
No kernel may reach another device: no remote copies, remote signals or barrier semaphores. Data moves between devices by JAX's collectives and lax.ppermute only.
A program may use at most 64 MiB of HBM per device.

```python
import math
import jax
import jax.numpy as jnp
from jax import lax

BLOCK = 128
SLOTS = 4
REACH = 2
NB_DEV = 512
E_DEV = 4096
GHOST = 192
NOFF = 4
BLOCKS = 16384
ELEMS = 131072
N_CURVE = 8
N_SEG = 4


def draw_slot_index(key, part):
    own_key = jax.random.fold_in(key, 11)
    pick_key = jax.random.fold_in(key, 12)
    ghost_key = jax.random.fold_in(key, 13)
    owned = jax.random.randint(own_key, (ELEMS, SLOTS), 0, NB_DEV)
    ghosts = NB_DEV + jax.random.randint(ghost_key, (ELEMS, SLOTS), 0, 2 * REACH * GHOST)
    picked = jax.random.randint(pick_key, (ELEMS, SLOTS), 0, 10) < 3
    picked = picked.at[:, 0].set(False)
    return jnp.where(picked, ghosts, owned).astype(jnp.int32)


def draw_slot_weight(key, part):
    table = jnp.array([-1, 3, 6, 8], dtype=jnp.int32)
    picks = jax.random.randint(jax.random.fold_in(key, 21), (ELEMS, SLOTS), 0, 4)
    codes = table[picks]
    return codes.at[:, 0].set(8).astype(jnp.int32)


def draw_ghost_live(key, part):
    devices_all = N_CURVE * N_SEG
    counts = jax.random.randint(jax.random.fold_in(key, 31), (devices_all, 2 * REACH), 0, GHOST + 1)
    device = jax.random.randint(jax.random.fold_in(key, 32), (), 0, devices_all)
    region = jax.random.randint(jax.random.fold_in(key, 33), (), 0, 2 * REACH)
    return counts.at[device, region].set(GHOST).astype(jnp.int32)


def draw_cell_count(key, part):
    devices_all = N_CURVE * N_SEG
    full = jax.random.randint(jax.random.fold_in(key, 41), (devices_all,), 0, 8) == 0
    shifts = jax.random.randint(jax.random.fold_in(key, 42), (devices_all,), 2, 4)
    counts = jnp.where(full, E_DEV, jnp.right_shift(jnp.full((devices_all,), E_DEV, jnp.int32), shifts))
    device = jax.random.randint(jax.random.fold_in(key, 43), (), 0, devices_all)
    return counts.at[device].set(E_DEV).astype(jnp.int32)


def set_ends(drawn, key, smallest, largest):
    longest = drawn.shape.index(max(drawn.shape))
    spots = []
    for shift in (0, 1):
        where = [jax.random.randint(jax.random.fold_in(key, axis), (), 0, length) for axis, length in enumerate(drawn.shape)]
        where[longest] = (where[longest] + shift) % drawn.shape[longest]
        spots.append(tuple(where))
    return drawn.at[spots[0]].set(smallest).at[spots[1]].set(largest)


def level_of(stream_key, extent, cuts, smallest, high):
    factor_of = 1.0
    for dim, shards_of in cuts:
        heights = jax.random.uniform(jax.random.fold_in(jax.random.fold_in(stream_key, 6), dim), (shards_of,), jnp.float32, smallest / len(cuts), high / len(cuts))
        factor_of = factor_of * jnp.repeat(jnp.exp(heights), extent[dim] // shards_of).reshape((-1,) + (1,) * (len(extent) - 1 - dim))
    return factor_of


def centred(stream_key, shape, scale, most, split=(), held_as=jnp.bfloat16):
    entries = scale * jax.random.normal(stream_key, shape, jnp.float32)
    if split:
        entries = entries * level_of(stream_key, shape, split, -0.22, 0.18)
    return jnp.clip(entries, -most, most).astype(held_as)


def setup_inputs(seed: int = 0) -> dict:
    keys = jax.random.split(jax.random.key(seed), 10)
    return {
        "solution": centred(keys[0], (BLOCKS, BLOCK), 1.0, 6.0, ((0, 32),)),
        "viscosity": jnp.clip(jnp.exp(math.log(10.0) - 4.6051702 * jax.random.uniform(keys[1], (ELEMS,), jnp.float32) ** level_of(keys[1], (ELEMS,), ((0, 32),), -0.2, 0.2)), 0.1, 10.0),
        "slot_index": draw_slot_index(jax.random.fold_in(keys[9], 71), 0),
        "slot_weight": draw_slot_weight(jax.random.fold_in(keys[9], 71), 0),
        "mirror_rows": set_ends(jax.random.randint(keys[4], (N_CURVE * N_SEG, NOFF, GHOST), 0, NB_DEV), jax.random.fold_in(keys[4], 1), 0, NB_DEV - 1).astype(jnp.int32),
        "ghost_live": draw_ghost_live(jax.random.fold_in(keys[9], 71), 0),
        "cell_count": draw_cell_count(jax.random.fold_in(keys[9], 71), 0),
        "viscous_block": centred(keys[7], (BLOCK, BLOCK), BLOCK ** -0.5, 0.5),
        "pressure_block": centred(keys[8], (BLOCK, BLOCK), BLOCK ** -0.5, 0.5),
    }


def shift_list(region_count):
    return [(region // 2 + 1) * (1 if region % 2 == 0 else -1) for region in range(region_count)]


def reference(solution, viscosity, slot_index, slot_weight, mirror_rows, ghost_live, cell_count, viscous_block, pressure_block):
    devices_all = N_CURVE * N_SEG
    offsets = shift_list(2 * REACH)
    owned_all = solution.reshape(devices_all, NB_DEV, BLOCK)
    ghost_pos = jnp.arange(GHOST, dtype=jnp.int32)
    elem_pos = jnp.arange(E_DEV, dtype=jnp.int32)

    def device_part(device):
        pieces = [owned_all[device]]
        for region, offset in enumerate(offsets):
            source = device - offset
            valid = (source >= 0) & (source < devices_all)
            sender = jnp.clip(source, 0, devices_all - 1).astype(jnp.int32)
            rows = owned_all[sender][mirror_rows[sender, region]]
            keep = valid & (ghost_pos < ghost_live[sender, region])
            pieces.append(jnp.where(keep[:, None], rows, jnp.zeros_like(rows)))
        extended = jnp.concatenate(pieces, axis=0)
        start = (device * E_DEV).astype(jnp.int32)
        indices = lax.dynamic_slice_in_dim(slot_index, start, E_DEV, 0)
        codes = lax.dynamic_slice_in_dim(slot_weight, start, E_DEV, 0)
        local_visc = lax.dynamic_slice_in_dim(viscosity, start, E_DEV, 0)
        live = (elem_pos < cell_count[device]).astype(jnp.float32)
        weights = codes.astype(jnp.float32) / 8.0 * live[:, None]
        element_in = jnp.zeros((E_DEV, BLOCK), jnp.float32)
        for slot_pos in range(SLOTS):
            element_in = element_in + weights[:, slot_pos, None] * extended[indices[:, slot_pos]].astype(jnp.float32)
        element_in = element_in.astype(jnp.bfloat16)
        element_out = local_visc[:, None] * jnp.dot(element_in, viscous_block, preferred_element_type=jnp.float32)
        element_out = element_out + jnp.dot(element_in, pressure_block, preferred_element_type=jnp.float32)
        partial_value = jnp.zeros((NB_DEV + 2 * REACH * GHOST, BLOCK), jnp.float32)
        for slot_pos in range(SLOTS):
            partial_value = partial_value.at[indices[:, slot_pos]].add(weights[:, slot_pos, None] * element_out)
        return partial_value[:NB_DEV], partial_value[NB_DEV:].reshape(2 * REACH, GHOST, BLOCK)

    owned_part, ghost_part = lax.map(device_part, jnp.arange(devices_all, dtype=jnp.int32))

    def finish(device):
        total = owned_part[device]
        for region, offset in enumerate(offsets):
            target = device + offset
            valid = (target >= 0) & (target < devices_all)
            holder = jnp.clip(target, 0, devices_all - 1).astype(jnp.int32)
            piece = ghost_part[holder, region]
            keep = valid & (ghost_pos < ghost_live[device, region])
            total = total.at[mirror_rows[device, region]].add(jnp.where(keep[:, None], piece, jnp.zeros_like(piece)))
        return total

    residual = lax.map(finish, jnp.arange(devices_all, dtype=jnp.int32))
    return residual.reshape(NB_DEV * devices_all, BLOCK)
```

```python
import functools

import jax
import jax.numpy as jnp
from jax import lax
from jax.experimental import pallas as pl
from jax.experimental.pallas import tpu as pltpu
from jax.sharding import PartitionSpec as P

AXES = ("curve", "seg")
PACK = 16
VMEM = pl.BlockSpec(memory_space=pltpu.VMEM)
SMEM = pl.BlockSpec(memory_space=pltpu.SMEM)


def matchings(region_count):
    return [(reach + 1, parity) for reach in range(region_count // 2) for parity in (0, 1)]


def exchange(block, distance, parity):
    total = lax.axis_size(AXES)
    route = []
    for d in range(total - distance):
        if (d // distance) % 2 == parity:
            route += [(d, d + distance), (d + distance, d)]
    return lax.ppermute(block, AXES, route)


def send_region(distance, parity):
    me = lax.axis_index("curve") * lax.axis_size("seg") + lax.axis_index("seg")
    up = (lax.div(me, distance) + parity) % 2
    return 2 * (distance - 1) + up


def one_hot_lists(mirror_ref, live_ref, region, rows):
    ghost = mirror_ref.shape[2]
    names = mirror_ref[0, pl.ds(region, 1), :]
    alive = lax.broadcasted_iota(jnp.int32, (1, ghost), 1) < live_ref[0, region]
    names = jnp.where(alive, names, -1)
    hit = lax.broadcasted_iota(jnp.int32, (rows, ghost), 0) == names
    return jnp.where(hit, 1.0, 0.0).astype(jnp.bfloat16)


def select_kernel(pairs, mirror_ref, live_ref, sol_ref, *out_refs):
    rows = sol_ref.shape[0]
    flipped = sol_ref[...].astype(jnp.float32).T.astype(jnp.bfloat16)
    for (distance, parity), out_ref in zip(pairs, out_refs):
        region = send_region(distance, parity)
        table = one_hot_lists(mirror_ref, live_ref, region, rows)
        picked = jnp.dot(flipped, table, preferred_element_type=jnp.float32)
        out_ref[...] = picked.T.astype(jnp.bfloat16)


def slot_rows(index_ref, weight_ref, count, start, width):
    slots = index_ref.shape[0]
    lanes = pl.ds(start, width)
    live = lax.broadcasted_iota(jnp.int32, (1, width), 1) + start < count
    names = [index_ref[pl.ds(i, 1), lanes] for i in range(slots)]
    codes = [weight_ref[pl.ds(i, 1), lanes] for i in range(slots)]
    sums = list(codes)
    for i in range(slots):
        for j in range(i + 1, slots):
            sums[i] = sums[i] + jnp.where(names[i] == names[j], codes[j], 0)
    out = []
    for i in range(slots):
        scaled = jnp.where(live, sums[i].astype(jnp.float32) * 0.125, 0.0)
        column = jnp.broadcast_to(names[i], (PACK, width)).astype(jnp.int16)
        weight = jnp.broadcast_to(scaled, (PACK, width)).astype(jnp.bfloat16)
        out.append((column, weight))
    return out


def selection(slots, base, rows, width):
    iota = lax.broadcasted_iota(jnp.int32, (PACK, width), 0)
    pieces = []
    for g in range(rows // PACK):
        here = (iota + (base + g * PACK)).astype(jnp.int16)
        piece = jnp.zeros((PACK, width), jnp.bfloat16)
        for column, weight in reversed(slots):
            piece = jnp.where(column == here, weight, piece)
        pieces.append(piece)
    return jnp.concatenate(pieces, axis=0)


def blocks_of(count, width):
    return lax.div(count + width - 1, width)


def gather_kernel(width, count_ref, index_ref, weight_ref, sol_ref, ein_ref):
    owned = sol_ref.shape[0]
    count = count_ref[0]
    flipped = sol_ref[...].astype(jnp.float32).T.astype(jnp.bfloat16)

    def body(b, carry):
        start = pl.multiple_of(b * width, width)
        slots = slot_rows(index_ref, weight_ref, count, start, width)
        table = selection(slots, 0, owned, width)
        ein_ref[:, pl.ds(start, width)] = jnp.dot(flipped, table, preferred_element_type=jnp.float32)
        return carry

    lax.fori_loop(0, blocks_of(count, width), body, 0)


def element_kernel(width, pairs, owned, count_ref, index_ref, weight_ref, visc_ref, ein_ref, mats_v_ref, mats_p_ref, *rest):
    n = len(pairs)
    ghost_refs, out_ref, ret_refs, (ghost_all, total) = rest[:n], rest[n], rest[n + 1 : 2 * n + 1], rest[2 * n + 1 :]
    ghost = ghost_refs[0].shape[0]
    count = count_ref[0]
    spots = []
    for (distance, parity), ghost_ref in zip(pairs, ghost_refs):
        sent = send_region(distance, parity)
        got = 4 * (distance - 1) + 1 - sent
        spot = pl.ds(pl.multiple_of(got * ghost, PACK), ghost)
        spots.append(spot)
        ghost_all[spot, :] = ghost_ref[...]
    flipped = ghost_all[...].astype(jnp.float32).T.astype(jnp.bfloat16)
    both = jnp.concatenate([mats_v_ref[...].astype(jnp.float32).T, mats_p_ref[...].astype(jnp.float32).T], axis=1).astype(jnp.bfloat16)
    total[...] = jnp.zeros_like(total)
    columns = n * ghost

    def body(b, carry):
        start = pl.multiple_of(b * width, width)
        lanes = pl.ds(start, width)
        slots = slot_rows(index_ref, weight_ref, count, start, width)[1:]
        table = selection(slots, owned, columns, width)
        ein = ein_ref[:, lanes] + jnp.dot(flipped, table, preferred_element_type=jnp.float32)
        stacked = jnp.concatenate([ein * visc_ref[:, lanes], ein], axis=0).astype(jnp.bfloat16)
        out = jnp.dot(both, stacked, preferred_element_type=jnp.float32).astype(jnp.bfloat16)
        out_ref[:, lanes] = out
        total[...] += lax.dot_general(table, out, (((1,), (1,)), ((), ())), preferred_element_type=jnp.float32)
        return carry

    lax.fori_loop(0, blocks_of(count, width), body, 0)
    for spot, ret_ref in zip(spots, ret_refs):
        ret_ref[...] = total[spot, :].astype(jnp.bfloat16)


def scatter_kernel(width, count_ref, index_ref, weight_ref, out_ref, part_ref):
    owned = part_ref.shape[0]
    count = count_ref[0]
    part_ref[...] = jnp.zeros_like(part_ref)

    def body(b, carry):
        start = pl.multiple_of(b * width, width)
        lanes = pl.ds(start, width)
        slots = slot_rows(index_ref, weight_ref, count, start, width)
        table = selection(slots, 0, owned, width)
        part_ref[...] += lax.dot_general(table, out_ref[:, lanes], (((1,), (1,)), ((), ())), preferred_element_type=jnp.float32)
        return carry

    lax.fori_loop(0, blocks_of(count, width), body, 0)


def finish_kernel(pairs, mirror_ref, live_ref, part_ref, *rest):
    back_refs, res_ref = rest[:-1], rest[-1]
    rows = part_ref.shape[0]
    total = part_ref[...]
    for (distance, parity), back_ref in zip(pairs, back_refs):
        region = send_region(distance, parity)
        table = one_hot_lists(mirror_ref, live_ref, region, rows)
        total = total + jnp.dot(table, back_ref[...], preferred_element_type=jnp.float32)
    res_ref[...] = total


def params(limit):
    return pltpu.CompilerParams(vmem_limit_bytes=limit * 1024 * 1024)


def cost(flops):
    return pl.CostEstimate(flops=flops, bytes_accessed=1 << 20, transcendentals=0)


def per_device(
    solution,
    viscosity,
    slot_index,
    slot_weight,
    mirror_rows,
    ghost_live,
    cell_count,
    viscous_block,
    pressure_block,
):
    owned, channels = solution.shape
    region_count, ghost = mirror_rows.shape[1:]
    elements = viscosity.shape[0]
    width = min(512, elements)
    pairs = matchings(region_count)
    index = slot_index.T
    weight = slot_weight.T
    visc = viscosity.reshape(1, elements)
    table_flops = 2 * elements * channels

    sent = pl.pallas_call(
        functools.partial(select_kernel, pairs),
        out_shape=[jax.ShapeDtypeStruct((ghost, channels), jnp.bfloat16)] * region_count,
        in_specs=[VMEM, SMEM, VMEM],
        out_specs=[VMEM] * region_count,
        compiler_params=params(16),
        cost_estimate=cost(2 * owned * channels * region_count * ghost),
        name="select",
    )(mirror_rows, ghost_live, solution)
    got = [exchange(block, *pair) for block, pair in zip(sent, pairs)]

    ein = pl.pallas_call(
        functools.partial(gather_kernel, width),
        out_shape=jax.ShapeDtypeStruct((channels, elements), jnp.float32),
        in_specs=[SMEM, VMEM, VMEM, VMEM],
        out_specs=VMEM,
        compiler_params=params(24),
        cost_estimate=cost(table_flops * owned * 8),
        name="gather_owned",
    )(cell_count, index, weight, solution)

    out, *ret = pl.pallas_call(
        functools.partial(element_kernel, width, pairs, owned),
        out_shape=[jax.ShapeDtypeStruct((channels, elements), jnp.bfloat16)]
        + [jax.ShapeDtypeStruct((ghost, channels), jnp.bfloat16)] * region_count,
        in_specs=[SMEM] + [VMEM] * (6 + region_count),
        out_specs=[VMEM] * (1 + region_count),
        scratch_shapes=[
            pltpu.VMEM((region_count * ghost, channels), jnp.bfloat16),
            pltpu.VMEM((region_count * ghost, channels), jnp.float32),
        ],
        compiler_params=params(24),
        cost_estimate=cost(table_flops * region_count * ghost * 2),
        name="elements",
    )(cell_count, index, weight, visc, ein, viscous_block, pressure_block, *got)
    back = [exchange(block, *pair) for block, pair in zip(ret, pairs)]

    part = pl.pallas_call(
        functools.partial(scatter_kernel, width),
        out_shape=jax.ShapeDtypeStruct((owned, channels), jnp.float32),
        in_specs=[SMEM, VMEM, VMEM, VMEM],
        out_specs=VMEM,
        compiler_params=params(24),
        cost_estimate=cost(table_flops * owned * 8),
        name="scatter_owned",
    )(cell_count, index, weight, out)

    return pl.pallas_call(
        functools.partial(finish_kernel, pairs),
        out_shape=jax.ShapeDtypeStruct((owned, channels), jnp.float32),
        in_specs=[VMEM, SMEM] + [VMEM] * (1 + region_count),
        out_specs=VMEM,
        compiler_params=params(16),
        cost_estimate=cost(2 * owned * channels * region_count * ghost),
        name="finish",
    )(mirror_rows, ghost_live, part, *back)


def solution(mesh):
    return jax.shard_map(
        per_device,
        mesh=mesh,
        in_specs=(
            P(AXES, None),
            P(AXES),
            P(AXES, None),
            P(AXES, None),
            P(AXES, None, None),
            P(AXES, None),
            P(AXES),
            P(),
            P(),
        ),
        out_specs=P(AXES, None),
        check_vma=False,
    )
```

```python
import functools

import jax
import jax.numpy as jnp
from jax import lax
from jax.experimental import pallas as pl
from jax.experimental.pallas import tpu as pltpu
from jax.sharding import PartitionSpec as P

AXES = ("curve", "seg")
PACK = 16
VMEM = pl.BlockSpec(memory_space=pltpu.VMEM)
SMEM = pl.BlockSpec(memory_space=pltpu.SMEM)
HBM = pl.BlockSpec(memory_space=pltpu.HBM)


def matchings(region_count):
    return [(reach + 1, parity) for reach in range(region_count // 2) for parity in (0, 1)]


def exchange(block, distance, parity):
    total = lax.axis_size(AXES)
    route = []
    for d in range(total - distance):
        if (d // distance) % 2 == parity:
            route += [(d, d + distance), (d + distance, d)]
    return lax.ppermute(block, AXES, route)


def send_region(distance, parity):
    me = lax.axis_index("curve") * lax.axis_size("seg") + lax.axis_index("seg")
    up = (lax.div(me, distance) + parity) % 2
    return 2 * (distance - 1) + up


def transposed(values):
    return values.astype(jnp.float32).T.astype(jnp.bfloat16)


def matmul(a, b):
    return jnp.dot(a, b, preferred_element_type=jnp.float32)


def matmul_nt(a, b):
    return lax.dot_general(a, b, (((1,), (1,)), ((), ())), preferred_element_type=jnp.float32)


def one_hot(names, rows):
    wide = jnp.broadcast_to(names, (PACK, names.shape[1])).astype(jnp.int16)
    iota = lax.broadcasted_iota(jnp.int32, wide.shape, 0)
    one, zero = jnp.ones(wide.shape, jnp.bfloat16), jnp.zeros(wide.shape, jnp.bfloat16)
    return jnp.concatenate([jnp.where(wide == (iota + g * PACK).astype(jnp.int16), one, zero) for g in range(rows // PACK)], axis=0)


def select_kernel(pairs, loads, mirror_hbm, live_hbm, sol_hbm, *rest):
    n = len(pairs)
    load_refs, rest = rest[:loads], rest[loads:]
    sent_refs, (names_ref, flipped_ref), rest = rest[:n], rest[n : n + 2], rest[n + 2 :]
    copy_refs, (mirror_ref, live_ref, sol_ref, sems) = rest[:loads], rest[loads:]
    first = [
        pltpu.make_async_copy(src, dst, sems.at[i])
        for i, (src, dst) in enumerate(((sol_hbm, sol_ref), (mirror_hbm, mirror_ref), (live_hbm, live_ref)))
    ]
    later = [pltpu.make_async_copy(src, dst, sems.at[len(first) + i]) for i, (src, dst) in enumerate(zip(load_refs, copy_refs))]
    for copy in first + later:
        copy.start()
    for copy in first:
        copy.wait()
    rows, ghost = sol_ref.shape[0], mirror_ref.shape[2]
    flipped = transposed(sol_ref[...])
    flipped_ref[...] = flipped
    lane = lax.broadcasted_iota(jnp.int32, (1, ghost), 1)
    for m, (distance, parity) in enumerate(pairs):
        region = send_region(distance, parity)
        names = jnp.where(lane < live_ref[0, region], mirror_ref[0, pl.ds(region, 1), :], -1)
        names_ref[pl.ds(m, 1), :] = names
        sent_refs[m][...] = matmul(flipped, one_hot(names, rows)).T.astype(jnp.bfloat16)
    for copy in later:
        copy.wait()


def slot_rows(index_ref, weight_ref, count_ref, start, width):
    slots = index_ref.shape[0]
    lanes = pl.ds(start, width)
    live = lax.broadcasted_iota(jnp.int32, (1, width), 1) + start < count_ref[0]
    names = [index_ref[pl.ds(i, 1), lanes] for i in range(slots)]
    codes = [weight_ref[pl.ds(i, 1), lanes] for i in range(slots)]
    sums = list(codes)
    for i in range(slots):
        for j in range(i + 1, slots):
            sums[i] = sums[i] + jnp.where(names[i] == names[j], codes[j], 0)
    out = []
    for i in range(slots):
        scaled = jnp.where(live, sums[i].astype(jnp.float32) * 0.125, 0.0)
        column = jnp.broadcast_to(names[i], (PACK, width)).astype(jnp.int16)
        weight = jnp.broadcast_to(scaled, (PACK, width)).astype(jnp.bfloat16)
        out.append((column, weight))
    return out


def selection(slots, base, rows, width):
    iota = lax.broadcasted_iota(jnp.int32, (PACK, width), 0)
    pieces = []
    for g in range(rows // PACK):
        here = (iota + (base + g * PACK)).astype(jnp.int16)
        piece = jnp.zeros((PACK, width), jnp.bfloat16)
        for column, weight in reversed(slots):
            piece = jnp.where(column == here, weight, piece)
        pieces.append(piece)
    return jnp.concatenate(pieces, axis=0)


def over_blocks(total, width, unroll, step):
    group = width * unroll

    def body(b, carry):
        for u in range(unroll):
            step(pl.multiple_of(b * group + u * width, width))
        return carry

    lax.fori_loop(0, total // group, body, 0)


def gather_kernel(width, unroll, count_ref, index_ref, weight_ref, flipped_ref, ein_ref, table_ref, turned_ref):
    owned, columns = flipped_ref.shape[1], table_ref.shape[0]

    def step(start):
        lanes = pl.ds(start, width)
        slots = slot_rows(index_ref, weight_ref, count_ref, start, width)
        ein_ref[:, lanes] = matmul(flipped_ref[...], selection(slots, 0, owned, width))
        table = selection(slots[1:], owned, columns, width)
        table_ref[:, lanes] = table
        turned_ref[lanes, :] = table.T

    over_blocks(ein_ref.shape[1], width, unroll, step)


def element_kernel(width, unroll, pairs, visc_ref, ein_ref, table_ref, turned_ref, mats_v_ref, mats_p_ref, *rest):
    n = len(pairs)
    ghost_refs, out_ref, ret_refs, (ghost_all, total, back) = rest[:n], rest[n], rest[n + 1 : 2 * n + 1], rest[2 * n + 1 :]
    ghost = ghost_refs[0].shape[0]
    spots = []
    for (distance, parity), ghost_ref in zip(pairs, ghost_refs):
        sent = send_region(distance, parity)
        got = 4 * (distance - 1) + 1 - sent
        spot = pl.ds(pl.multiple_of(got * ghost, PACK), ghost)
        spots.append(spot)
        ghost_all[spot, :] = ghost_ref[...]
    flipped = transposed(ghost_all[...])
    both = jnp.concatenate([mats_v_ref[...].astype(jnp.float32).T, mats_p_ref[...].astype(jnp.float32).T], axis=1).astype(jnp.bfloat16)
    total[...] = jnp.zeros_like(total)

    def step(start):
        lanes = pl.ds(start, width)
        ein = ein_ref[:, lanes] + matmul(flipped, table_ref[:, lanes])
        stacked = jnp.concatenate([ein * visc_ref[:, lanes], ein], axis=0).astype(jnp.bfloat16)
        out = matmul(both, stacked).astype(jnp.bfloat16)
        out_ref[:, lanes] = out
        total[...] += matmul(out, turned_ref[lanes, :])

    over_blocks(ein_ref.shape[1], width, unroll, step)
    back[...] = total[...].T
    for spot, ret_ref in zip(spots, ret_refs):
        ret_ref[...] = back[spot, :].astype(jnp.bfloat16)


def scatter_kernel(width, unroll, count_ref, index_ref, weight_ref, out_ref, names_ref, part_ref, *hit_refs):
    owned = part_ref.shape[0]
    part_ref[...] = jnp.zeros_like(part_ref)
    for m, hit_ref in enumerate(hit_refs):
        hit_ref[...] = one_hot(names_ref[pl.ds(m, 1), :], owned)

    def step(start):
        lanes = pl.ds(start, width)
        slots = slot_rows(index_ref, weight_ref, count_ref, start, width)
        part_ref[...] += matmul_nt(selection(slots, 0, owned, width), out_ref[:, lanes])

    over_blocks(out_ref.shape[1], width, unroll, step)


def finish_kernel(n, part_ref, *rest):
    hit_refs, back_refs, res_ref = rest[:n], rest[n : 2 * n], rest[2 * n]
    total = part_ref[...]
    for hit_ref, back_ref in zip(hit_refs, back_refs):
        total = total + matmul(hit_ref[...], back_ref[...])
    res_ref[...] = total


def params(limit):
    return pltpu.CompilerParams(vmem_limit_bytes=limit * 1024 * 1024)


def cost(flops):
    return pl.CostEstimate(flops=flops, bytes_accessed=1 << 20, transcendentals=0)


def like(*arrays):
    return [jax.ShapeDtypeStruct(a.shape, a.dtype) for a in arrays]


def per_device(
    solution,
    viscosity,
    slot_index,
    slot_weight,
    mirror_rows,
    ghost_live,
    cell_count,
    viscous_block,
    pressure_block,
):
    owned, channels = solution.shape
    regions, ghost = mirror_rows.shape[1:]
    elements = viscosity.shape[0]
    width = min(512, elements)
    unroll = min(4, elements // width)
    pairs = matchings(regions)
    bf16, f32 = jnp.bfloat16, jnp.float32
    table_flops = 2 * elements * channels
    list_shape = [jax.ShapeDtypeStruct((ghost, channels), bf16)] * regions
    loads = [slot_index.T, slot_weight.T, viscosity.reshape(1, elements), viscous_block, pressure_block]

    outs = pl.pallas_call(
        functools.partial(select_kernel, pairs, len(loads)),
        out_shape=list_shape
        + [
            jax.ShapeDtypeStruct((regions, ghost), jnp.int32),
            jax.ShapeDtypeStruct((channels, owned), bf16),
        ]
        + like(*loads),
        in_specs=[HBM] * (3 + len(loads)),
        out_specs=[VMEM] * (regions + 2 + len(loads)),
        scratch_shapes=[
            pltpu.VMEM(mirror_rows.shape, jnp.int32),
            pltpu.SMEM(ghost_live.shape, jnp.int32),
            pltpu.VMEM(solution.shape, bf16),
            pltpu.SemaphoreType.DMA((3 + len(loads),)),
        ],
        compiler_params=params(16),
        cost_estimate=cost(2 * owned * channels * regions * ghost),
        name="select",
    )(*[pltpu.with_memory_space_constraint(a, pltpu.HBM) for a in (mirror_rows, ghost_live, solution, *loads)])
    sent, (names, flipped, index, weight, visc, mats_v, mats_p) = outs[:regions], outs[regions:]
    got = [exchange(block, *pair) for block, pair in zip(sent, pairs)]

    ein, table, turned = pl.pallas_call(
        functools.partial(gather_kernel, width, unroll),
        out_shape=[
            jax.ShapeDtypeStruct((channels, elements), f32),
            jax.ShapeDtypeStruct((regions * ghost, elements), bf16),
            jax.ShapeDtypeStruct((elements, regions * ghost), bf16),
        ],
        in_specs=[SMEM] + [VMEM] * 3,
        out_specs=[VMEM] * 3,
        compiler_params=params(20),
        cost_estimate=cost(table_flops * owned * 8),
        name="gather_owned",
    )(cell_count, index, weight, flipped)

    out, *ret = pl.pallas_call(
        functools.partial(element_kernel, width, unroll, pairs),
        out_shape=[jax.ShapeDtypeStruct((channels, elements), bf16)] + list_shape,
        in_specs=[VMEM] * (6 + regions),
        out_specs=[VMEM] * (1 + regions),
        scratch_shapes=[
            pltpu.VMEM((regions * ghost, channels), bf16),
            pltpu.VMEM((channels, regions * ghost), f32),
            pltpu.VMEM((regions * ghost, channels), f32),
        ],
        compiler_params=params(20),
        cost_estimate=cost(table_flops * regions * ghost * 2),
        name="elements",
    )(visc, ein, table, turned, mats_v, mats_p, *got)
    back = [exchange(block, *pair) for block, pair in zip(ret, pairs)]

    part, *hits = pl.pallas_call(
        functools.partial(scatter_kernel, width, unroll),
        out_shape=[jax.ShapeDtypeStruct((owned, channels), f32)] + [jax.ShapeDtypeStruct((owned, ghost), bf16)] * regions,
        in_specs=[SMEM] + [VMEM] * 4,
        out_specs=[VMEM] * (1 + regions),
        compiler_params=params(20),
        cost_estimate=cost(table_flops * owned * 8),
        name="scatter_owned",
    )(cell_count, index, weight, out, names)

    return pl.pallas_call(
        functools.partial(finish_kernel, regions),
        out_shape=jax.ShapeDtypeStruct((owned, channels), f32),
        in_specs=[VMEM] * (1 + 2 * regions),
        out_specs=VMEM,
        compiler_params=params(16),
        cost_estimate=cost(2 * owned * channels * regions * ghost),
        name="finish",
    )(part, *hits, *back)


def solution(mesh):
    return jax.shard_map(
        per_device,
        mesh=mesh,
        in_specs=(
            P(AXES, None),
            P(AXES),
            P(AXES, None),
            P(AXES, None),
            P(AXES, None, None),
            P(AXES, None),
            P(AXES),
            P(),
            P(),
        ),
        out_specs=P(AXES, None),
        check_vma=False,
    )
```

```python
import functools

import jax
import jax.numpy as jnp
from jax import lax
from jax.experimental import pallas as pl
from jax.experimental.pallas import tpu as pltpu
from jax.sharding import PartitionSpec as P

AXES = ("curve", "seg")
PACK = 16
VMEM = pl.BlockSpec(memory_space=pltpu.VMEM)
SMEM = pl.BlockSpec(memory_space=pltpu.SMEM)
HBM = pl.BlockSpec(memory_space=pltpu.HBM)


def matchings(region_count):
    return [(reach + 1, parity) for parity in (1, 0) for reach in reversed(range(region_count // 2))]


def exchange(block, distance, parity):
    total = lax.axis_size(AXES)
    route = []
    for d in range(total - distance):
        if (d // distance) % 2 == parity:
            route += [(d, d + distance), (d + distance, d)]
    return lax.ppermute(block, AXES, route)


def send_region(distance, parity):
    me = lax.axis_index("curve") * lax.axis_size("seg") + lax.axis_index("seg")
    up = (lax.div(me, distance) + parity) % 2
    return 2 * (distance - 1) + up


def transposed(values):
    return values.astype(jnp.float32).T.astype(jnp.bfloat16)


def matmul(a, b):
    return jnp.dot(a, b, preferred_element_type=jnp.float32)


def matmul_nt(a, b):
    return lax.dot_general(a, b, (((1,), (1,)), ((), ())), preferred_element_type=jnp.float32)


def one_hot(names, rows):
    wide = jnp.broadcast_to(names, (PACK, names.shape[1])).astype(jnp.int16)
    iota = lax.broadcasted_iota(jnp.int32, wide.shape, 0)
    one, zero = jnp.ones(wide.shape, jnp.bfloat16), jnp.zeros(wide.shape, jnp.bfloat16)
    return jnp.concatenate([jnp.where(wide == (iota + g * PACK).astype(jnp.int16), one, zero) for g in range(rows // PACK)], axis=0)


def select_kernel(pairs, loads, mirror_hbm, live_hbm, sol_hbm, *rest):
    n = len(pairs)
    load_refs, rest = rest[:loads], rest[loads:]
    sent_refs, (names_ref, flipped_ref), rest = rest[:n], rest[n : n + 2], rest[n + 2 :]
    copy_refs, (mirror_ref, live_ref, sol_ref, sems) = rest[:loads], rest[loads:]
    first = [
        pltpu.make_async_copy(src, dst, sems.at[i])
        for i, (src, dst) in enumerate(((sol_hbm, sol_ref), (mirror_hbm, mirror_ref), (live_hbm, live_ref)))
    ]
    later = [pltpu.make_async_copy(src, dst, sems.at[len(first) + i]) for i, (src, dst) in enumerate(zip(load_refs, copy_refs))]
    for copy in first + later:
        copy.start()
    for copy in first:
        copy.wait()
    rows, ghost = sol_ref.shape[0], mirror_ref.shape[2]
    flipped = transposed(sol_ref[...])
    flipped_ref[...] = flipped
    lane = lax.broadcasted_iota(jnp.int32, (1, ghost), 1)
    for m, (distance, parity) in enumerate(pairs):
        region = send_region(distance, parity)
        names = jnp.where(lane < live_ref[0, region], mirror_ref[0, pl.ds(region, 1), :], -1)
        names_ref[pl.ds(m, 1), :] = names
        sent_refs[m][...] = matmul(flipped, one_hot(names, rows)).T.astype(jnp.bfloat16)
    for copy in later:
        copy.wait()


def slot_rows(index_ref, weight_ref, count, lanes):
    slots, width = index_ref.shape[0], lanes.size
    live = lax.broadcasted_iota(jnp.int32, (1, width), 1) + lanes.start < count
    names = [index_ref[pl.ds(i, 1), lanes] for i in range(slots)]
    codes = [weight_ref[pl.ds(i, 1), lanes] for i in range(slots)]
    sums = list(codes)
    for i in range(slots):
        for j in range(i + 1, slots):
            sums[i] = sums[i] + jnp.where(names[i] == names[j], codes[j], 0)
    out = []
    for i in range(slots):
        scaled = jnp.where(live, sums[i].astype(jnp.float32) * 0.125, 0.0)
        column = jnp.broadcast_to(names[i], (PACK, width)).astype(jnp.int16)
        weight = jnp.broadcast_to(scaled, (PACK, width)).astype(jnp.bfloat16)
        out.append((column, weight))
    return out


def load_rows(column_ref, share_ref, lanes, first):
    slots = column_ref.shape[0] // PACK
    return [(column_ref[i * PACK : (i + 1) * PACK, lanes], share_ref[i * PACK : (i + 1) * PACK, lanes]) for i in range(first, slots)]


def selection(slots, base, rows):
    shape = slots[0][0].shape
    iota = lax.broadcasted_iota(jnp.int32, shape, 0)
    pieces = []
    for g in range(rows // PACK):
        here = (iota + (base + g * PACK)).astype(jnp.int16)
        piece = jnp.zeros(shape, jnp.bfloat16)
        for column, weight in reversed(slots):
            piece = jnp.where(column == here, weight, piece)
        pieces.append(piece)
    return jnp.concatenate(pieces, axis=0)


def lane_blocks(total, width):
    return [pl.ds(start, width) for start in range(0, total, width)]


def gather_kernel(width, count_ref, index_ref, weight_ref, flipped_ref, ein_ref, column_ref, share_ref, table_ref, turned_ref):
    owned, columns = flipped_ref.shape[1], table_ref.shape[0]
    for lanes in lane_blocks(ein_ref.shape[1], width):
        slots = slot_rows(index_ref, weight_ref, count_ref[0], lanes)
        for i, (column, share) in enumerate(slots):
            column_ref[i * PACK : (i + 1) * PACK, lanes] = column
            share_ref[i * PACK : (i + 1) * PACK, lanes] = share
        ein_ref[:, lanes] = matmul(flipped_ref[...], selection(slots, 0, owned))
        if lanes.start < table_ref.shape[1]:
            table = selection(slots[1:], owned, columns)
            table_ref[:, lanes] = table
            turned_ref[lanes, :] = table.T


def element_kernel(width, pairs, owned, visc_ref, ein_ref, column_ref, share_ref, table_ref, turned_ref, mats_v_ref, mats_p_ref, *rest):
    n = len(pairs)
    ghost_refs, out_ref, ret_refs, rest = rest[:n], rest[n], rest[n + 1 : 2 * n + 1], rest[2 * n + 1 :]
    ghost_all, stacked_ref, late_ref, back = rest
    ghost, channels = ghost_refs[0].shape
    early, columns = table_ref.shape[1], table_ref.shape[0]
    blocks = lane_blocks(ein_ref.shape[1], width)
    spots = []
    for (distance, parity), ghost_ref in zip(pairs, ghost_refs):
        sent = send_region(distance, parity)
        got = 4 * (distance - 1) + 1 - sent
        spot = pl.ds(pl.multiple_of(got * ghost, PACK), ghost)
        spots.append(spot)
        ghost_all[spot, :] = ghost_ref[...]
    flipped = transposed(ghost_all[...])
    both = jnp.concatenate([mats_v_ref[...].astype(jnp.float32).T, mats_p_ref[...].astype(jnp.float32).T], axis=1).astype(jnp.bfloat16)
    for lanes in blocks:
        if lanes.start < early:
            table = table_ref[:, lanes]
        else:
            table = selection(load_rows(column_ref, share_ref, lanes, 1), owned, columns)
            late_ref[pl.ds(lanes.start - early, width), :] = table.T
        ein = ein_ref[:, lanes] + matmul(flipped, table)
        stacked_ref[:channels, lanes] = (ein * visc_ref[:, lanes]).astype(jnp.bfloat16)
        stacked_ref[channels:, lanes] = ein.astype(jnp.bfloat16)
    for lanes in blocks:
        out_ref[:, lanes] = matmul(both, stacked_ref[:, lanes]).astype(jnp.bfloat16)
    total = matmul(out_ref[:, :early], turned_ref[...])
    if early < ein_ref.shape[1]:
        total = total + matmul(out_ref[:, early:], late_ref[...])
    back[...] = total.T
    for spot, ret_ref in zip(spots, ret_refs):
        ret_ref[...] = back[spot, :].astype(jnp.bfloat16)


def scatter_kernel(width, column_ref, share_ref, out_ref, names_ref, part_ref, *rest):
    hit_refs, turned_ref = rest[:-1], rest[-1]
    owned = part_ref.shape[0]
    for lanes in lane_blocks(out_ref.shape[1], width):
        turned_ref[lanes, :] = selection(load_rows(column_ref, share_ref, lanes, 0), 0, owned).T
    part_ref[...] = matmul(out_ref[...], turned_ref[...]).T
    for m, hit_ref in enumerate(hit_refs):
        hit_ref[...] = one_hot(names_ref[pl.ds(m, 1), :], owned)


def finish_kernel(n, part_ref, *rest):
    hit_refs, back_refs, res_ref = rest[:n], rest[n : 2 * n], rest[2 * n]
    total = part_ref[...]
    for hit_ref, back_ref in zip(hit_refs, back_refs):
        total = total + matmul(hit_ref[...], back_ref[...])
    res_ref[...] = total


def params(limit):
    return pltpu.CompilerParams(vmem_limit_bytes=limit * 1024 * 1024)


def cost(flops):
    return pl.CostEstimate(flops=flops, bytes_accessed=1 << 20, transcendentals=0)


def like(*arrays):
    return [jax.ShapeDtypeStruct(a.shape, a.dtype) for a in arrays]


def per_device(
    solution,
    viscosity,
    slot_index,
    slot_weight,
    mirror_rows,
    ghost_live,
    cell_count,
    viscous_block,
    pressure_block,
):
    owned, channels = solution.shape
    regions, ghost = mirror_rows.shape[1:]
    elements = viscosity.shape[0]
    width = min(512, elements)
    early = elements // 2
    slots = slot_index.shape[1]
    pairs = matchings(regions)
    bf16, f32 = jnp.bfloat16, jnp.float32
    table_flops = 2 * elements * channels
    list_shape = [jax.ShapeDtypeStruct((ghost, channels), bf16)] * regions
    loads = [slot_index.T, slot_weight.T, viscosity.reshape(1, elements), viscous_block, pressure_block]

    outs = pl.pallas_call(
        functools.partial(select_kernel, pairs, len(loads)),
        out_shape=list_shape
        + [
            jax.ShapeDtypeStruct((regions, ghost), jnp.int32),
            jax.ShapeDtypeStruct((channels, owned), bf16),
        ]
        + like(*loads),
        in_specs=[HBM] * (3 + len(loads)),
        out_specs=[VMEM] * (regions + 2 + len(loads)),
        scratch_shapes=[
            pltpu.VMEM(mirror_rows.shape, jnp.int32),
            pltpu.SMEM(ghost_live.shape, jnp.int32),
            pltpu.VMEM(solution.shape, bf16),
            pltpu.SemaphoreType.DMA((3 + len(loads),)),
        ],
        compiler_params=params(16),
        cost_estimate=cost(2 * owned * channels * regions * ghost),
        name="select",
    )(*[pltpu.with_memory_space_constraint(a, pltpu.HBM) for a in (mirror_rows, ghost_live, solution, *loads)])
    sent, (names, flipped, index, weight, visc, mats_v, mats_p) = outs[:regions], outs[regions:]
    got = [exchange(block, *pair) for block, pair in zip(sent, pairs)]

    ein, column, share, table, turned = pl.pallas_call(
        functools.partial(gather_kernel, width),
        out_shape=[
            jax.ShapeDtypeStruct((channels, elements), f32),
            jax.ShapeDtypeStruct((PACK * slots, elements), jnp.int16),
            jax.ShapeDtypeStruct((PACK * slots, elements), bf16),
            jax.ShapeDtypeStruct((regions * ghost, early), bf16),
            jax.ShapeDtypeStruct((early, regions * ghost), bf16),
        ],
        in_specs=[SMEM] + [VMEM] * 3,
        out_specs=[VMEM] * 5,
        compiler_params=params(20),
        cost_estimate=cost(table_flops * owned * 8),
        name="gather_owned",
    )(cell_count, index, weight, flipped)

    out, *ret = pl.pallas_call(
        functools.partial(element_kernel, width, pairs, owned),
        out_shape=[jax.ShapeDtypeStruct((channels, elements), bf16)] + list_shape,
        in_specs=[VMEM] * (8 + regions),
        out_specs=[VMEM] * (1 + regions),
        scratch_shapes=[
            pltpu.VMEM((regions * ghost, channels), bf16),
            pltpu.VMEM((2 * channels, elements), bf16),
            pltpu.VMEM((max(elements - early, PACK), regions * ghost), bf16),
            pltpu.VMEM((regions * ghost, channels), f32),
        ],
        compiler_params=params(24),
        cost_estimate=cost(table_flops * regions * ghost * 2),
        name="elements",
    )(visc, ein, column, share, table, turned, mats_v, mats_p, *got)
    back = [exchange(block, *pair) for block, pair in zip(ret, pairs)]

    part, *hits = pl.pallas_call(
        functools.partial(scatter_kernel, width),
        out_shape=[jax.ShapeDtypeStruct((owned, channels), f32)] + [jax.ShapeDtypeStruct((owned, ghost), bf16)] * regions,
        in_specs=[VMEM] * 4,
        out_specs=[VMEM] * (1 + regions),
        scratch_shapes=[pltpu.VMEM((elements, owned), bf16)],
        compiler_params=params(24),
        cost_estimate=cost(table_flops * owned * 8),
        name="scatter_owned",
    )(column, share, out, names)

    return pl.pallas_call(
        functools.partial(finish_kernel, regions),
        out_shape=jax.ShapeDtypeStruct((owned, channels), f32),
        in_specs=[VMEM] * (1 + 2 * regions),
        out_specs=VMEM,
        compiler_params=params(16),
        cost_estimate=cost(2 * owned * channels * regions * ghost),
        name="finish",
    )(part, *hits, *back)


def solution(mesh):
    return jax.shard_map(
        per_device,
        mesh=mesh,
        in_specs=(
            P(AXES, None),
            P(AXES),
            P(AXES, None),
            P(AXES, None),
            P(AXES, None, None),
            P(AXES, None),
            P(AXES),
            P(),
            P(),
        ),
        out_specs=P(AXES, None),
        check_vma=False,
    )
```

```python
import functools

import jax
import jax.numpy as jnp
from jax import lax
from jax.experimental import pallas as pl
from jax.experimental.pallas import tpu as pltpu
from jax.sharding import PartitionSpec as P

AXES = ("curve", "seg")
PACK = 16
VMEM = pl.BlockSpec(memory_space=pltpu.VMEM)
SMEM = pl.BlockSpec(memory_space=pltpu.SMEM)
HBM = pl.BlockSpec(memory_space=pltpu.HBM)


def matchings(region_count):
    reaches = range(1, region_count // 2 + 1)
    return [(reach, 1) for reach in reaches] + [(reach, 0) for reach in reversed(reaches)]


def exchange(block, distance, parity):
    total = lax.axis_size(AXES)
    swaps = [(d, d + distance) for d in range(total - distance) if (d // distance) % 2 == parity]
    left = sorted(set(range(total)) - {d for swap in swaps for d in swap})
    swaps += list(zip(left[::2], left[1::2]))
    return lax.ppermute(block, AXES, swaps + [(b, a) for a, b in swaps])


def send_region(distance, parity):
    seg = lax.axis_size("seg")
    me = lax.axis_index("curve") * seg + lax.axis_index("seg")
    down = (lax.div(me, distance) + parity) % 2
    there = me + distance * (1 - 2 * down)
    return 2 * (distance - 1) + down, (there >= 0) & (there < seg * lax.axis_size("curve"))


def transposed(values):
    return values.astype(jnp.float32).T.astype(jnp.bfloat16)


def matmul(a, b):
    return jnp.dot(a, b, preferred_element_type=jnp.float32)


def matmul_nt(a, b):
    return lax.dot_general(a, b, (((1,), (1,)), ((), ())), preferred_element_type=jnp.float32)


def one_hot(names, rows):
    wide = jnp.broadcast_to(names, (PACK, names.shape[1])).astype(jnp.int16)
    iota = lax.broadcasted_iota(jnp.int32, wide.shape, 0)
    one, zero = jnp.ones(wide.shape, jnp.bfloat16), jnp.zeros(wide.shape, jnp.bfloat16)
    return jnp.concatenate([jnp.where(wide == (iota + g * PACK).astype(jnp.int16), one, zero) for g in range(rows // PACK)], axis=0)


def select_kernel(pairs, loads, mirror_hbm, live_hbm, sol_hbm, *rest):
    n = len(pairs)
    load_refs, rest = rest[:loads], rest[loads:]
    sent_refs, (names_ref, flipped_ref), rest = rest[:n], rest[n : n + 2], rest[n + 2 :]
    copy_refs, (mirror_ref, live_ref, sol_ref, sems) = rest[:loads], rest[loads:]
    first = [
        pltpu.make_async_copy(src, dst, sems.at[i])
        for i, (src, dst) in enumerate(((sol_hbm, sol_ref), (mirror_hbm, mirror_ref), (live_hbm, live_ref)))
    ]
    later = [pltpu.make_async_copy(src, dst, sems.at[len(first) + i]) for i, (src, dst) in enumerate(zip(load_refs, copy_refs))]
    for copy in first + later:
        copy.start()
    for copy in first:
        copy.wait()
    rows, ghost = sol_ref.shape[0], mirror_ref.shape[2]
    flipped = transposed(sol_ref[...])
    flipped_ref[...] = flipped
    lane = lax.broadcasted_iota(jnp.int32, (1, ghost), 1)
    for m, (distance, parity) in enumerate(pairs):
        region, there = send_region(distance, parity)
        names = jnp.where(lane < jnp.where(there, live_ref[0, region], 0), mirror_ref[0, pl.ds(region, 1), :], -1)
        names_ref[pl.ds(m, 1), :] = names
        sent_refs[m][...] = matmul(flipped, one_hot(names, rows)).T.astype(jnp.bfloat16)
    for copy in later:
        copy.wait()


def slot_rows(index_ref, weight_ref, count, lanes):
    slots, width = index_ref.shape[0], lanes.size
    live = lax.broadcasted_iota(jnp.int32, (1, width), 1) + lanes.start < count
    names = [index_ref[pl.ds(i, 1), lanes] for i in range(slots)]
    codes = [weight_ref[pl.ds(i, 1), lanes] for i in range(slots)]
    sums = list(codes)
    for i in range(slots):
        for j in range(i + 1, slots):
            sums[i] = sums[i] + jnp.where(names[i] == names[j], codes[j], 0)
    out = []
    for i in range(slots):
        scaled = jnp.where(live, sums[i].astype(jnp.float32) * 0.125, 0.0)
        column = jnp.broadcast_to(names[i], (PACK, width)).astype(jnp.int16)
        weight = jnp.broadcast_to(scaled, (PACK, width)).astype(jnp.bfloat16)
        out.append((column, weight))
    return out


def load_rows(column_ref, share_ref, lanes, first):
    slots = column_ref.shape[0] // PACK
    return [(column_ref[i * PACK : (i + 1) * PACK, lanes], share_ref[i * PACK : (i + 1) * PACK, lanes]) for i in range(first, slots)]


def selection(slots, base, rows):
    shape = slots[0][0].shape
    iota = lax.broadcasted_iota(jnp.int32, shape, 0)
    pieces = []
    for g in range(rows // PACK):
        here = (iota + (base + g * PACK)).astype(jnp.int16)
        piece = jnp.zeros(shape, jnp.bfloat16)
        for column, weight in reversed(slots):
            piece = jnp.where(column == here, weight, piece)
        pieces.append(piece)
    return jnp.concatenate(pieces, axis=0)


def lane_blocks(total, width):
    return [pl.ds(start, width) for start in range(0, total, width)]


def gather_kernel(width, count_ref, index_ref, weight_ref, flipped_ref, ein_ref, column_ref, share_ref, table_ref, turned_ref):
    owned, columns = flipped_ref.shape[1], table_ref.shape[0]
    for lanes in lane_blocks(ein_ref.shape[1], width):
        slots = slot_rows(index_ref, weight_ref, count_ref[0], lanes)
        for i, (column, share) in enumerate(slots):
            column_ref[i * PACK : (i + 1) * PACK, lanes] = column
            share_ref[i * PACK : (i + 1) * PACK, lanes] = share
        ein_ref[:, lanes] = matmul(flipped_ref[...], selection(slots, 0, owned))
        if lanes.start < table_ref.shape[1]:
            table = selection(slots[1:], owned, columns)
            table_ref[:, lanes] = table
            turned_ref[lanes, :] = table.T


def element_kernel(width, pairs, owned, visc_ref, ein_ref, column_ref, share_ref, table_ref, turned_ref, mats_v_ref, mats_p_ref, *rest):
    n = len(pairs)
    ghost_refs, out_ref, ret_refs, rest = rest[:n], rest[n], rest[n + 1 : 2 * n + 1], rest[2 * n + 1 :]
    ghost_all, stacked_ref, late_ref, back = rest
    ghost, channels = ghost_refs[0].shape
    early, columns = table_ref.shape[1], table_ref.shape[0]
    blocks = lane_blocks(ein_ref.shape[1], width)
    spots = []
    for (distance, parity), ghost_ref in zip(pairs, ghost_refs):
        sent, _ = send_region(distance, parity)
        got = 4 * (distance - 1) + 1 - sent
        spot = pl.ds(pl.multiple_of(got * ghost, PACK), ghost)
        spots.append(spot)
        ghost_all[spot, :] = ghost_ref[...]
    flipped = transposed(ghost_all[...])
    both = jnp.concatenate([mats_v_ref[...].astype(jnp.float32).T, mats_p_ref[...].astype(jnp.float32).T], axis=1).astype(jnp.bfloat16)
    for lanes in blocks:
        if lanes.start < early:
            table = table_ref[:, lanes]
        else:
            table = selection(load_rows(column_ref, share_ref, lanes, 1), owned, columns)
            late_ref[pl.ds(lanes.start - early, width), :] = table.T
        ein = ein_ref[:, lanes] + matmul(flipped, table)
        stacked_ref[:channels, lanes] = (ein * visc_ref[:, lanes]).astype(jnp.bfloat16)
        stacked_ref[channels:, lanes] = ein.astype(jnp.bfloat16)
    for lanes in blocks:
        out_ref[:, lanes] = matmul(both, stacked_ref[:, lanes]).astype(jnp.bfloat16)
    total = matmul(out_ref[:, :early], turned_ref[...])
    if early < ein_ref.shape[1]:
        total = total + matmul(out_ref[:, early:], late_ref[...])
    back[...] = total.T
    for spot, ret_ref in zip(spots, ret_refs):
        ret_ref[...] = back[spot, :].astype(jnp.bfloat16)


def scatter_kernel(width, column_ref, share_ref, out_ref, names_ref, part_ref, *rest):
    hit_refs, turned_ref = rest[:-1], rest[-1]
    owned = part_ref.shape[0]
    for lanes in lane_blocks(out_ref.shape[1], width):
        turned_ref[lanes, :] = selection(load_rows(column_ref, share_ref, lanes, 0), 0, owned).T
    part_ref[...] = matmul(out_ref[...], turned_ref[...]).T
    for m, hit_ref in enumerate(hit_refs):
        hit_ref[...] = one_hot(names_ref[pl.ds(m, 1), :], owned)


def finish_kernel(n, part_ref, *rest):
    hit_refs, back_refs, res_ref = rest[:n], rest[n : 2 * n], rest[2 * n]
    total = part_ref[...]
    for hit_ref, back_ref in zip(hit_refs, back_refs):
        total = total + matmul(hit_ref[...], back_ref[...])
    res_ref[...] = total


def params(limit):
    return pltpu.CompilerParams(vmem_limit_bytes=limit * 1024 * 1024)


def cost(flops):
    return pl.CostEstimate(flops=flops, bytes_accessed=1 << 20, transcendentals=0)


def like(*arrays):
    return [jax.ShapeDtypeStruct(a.shape, a.dtype) for a in arrays]


def per_device(
    solution,
    viscosity,
    slot_index,
    slot_weight,
    mirror_rows,
    ghost_live,
    cell_count,
    viscous_block,
    pressure_block,
):
    owned, channels = solution.shape
    regions, ghost = mirror_rows.shape[1:]
    elements = viscosity.shape[0]
    width = min(512, elements)
    early = elements // 2
    slots = slot_index.shape[1]
    pairs = matchings(regions)
    bf16, f32 = jnp.bfloat16, jnp.float32
    table_flops = 2 * elements * channels
    list_shape = [jax.ShapeDtypeStruct((ghost, channels), bf16)] * regions
    loads = [slot_index.T, slot_weight.T, viscosity.reshape(1, elements), viscous_block, pressure_block]

    outs = pl.pallas_call(
        functools.partial(select_kernel, pairs, len(loads)),
        out_shape=list_shape
        + [
            jax.ShapeDtypeStruct((regions, ghost), jnp.int32),
            jax.ShapeDtypeStruct((channels, owned), bf16),
        ]
        + like(*loads),
        in_specs=[HBM] * (3 + len(loads)),
        out_specs=[VMEM] * (regions + 2 + len(loads)),
        scratch_shapes=[
            pltpu.VMEM(mirror_rows.shape, jnp.int32),
            pltpu.SMEM(ghost_live.shape, jnp.int32),
            pltpu.VMEM(solution.shape, bf16),
            pltpu.SemaphoreType.DMA((3 + len(loads),)),
        ],
        compiler_params=params(16),
        cost_estimate=cost(2 * owned * channels * regions * ghost),
        name="select",
    )(*[pltpu.with_memory_space_constraint(a, pltpu.HBM) for a in (mirror_rows, ghost_live, solution, *loads)])
    sent, (names, flipped, index, weight, visc, mats_v, mats_p) = outs[:regions], outs[regions:]
    got = [exchange(block, *pair) for block, pair in zip(sent, pairs)]

    ein, column, share, table, turned = pl.pallas_call(
        functools.partial(gather_kernel, width),
        out_shape=[
            jax.ShapeDtypeStruct((channels, elements), f32),
            jax.ShapeDtypeStruct((PACK * slots, elements), jnp.int16),
            jax.ShapeDtypeStruct((PACK * slots, elements), bf16),
            jax.ShapeDtypeStruct((regions * ghost, early), bf16),
            jax.ShapeDtypeStruct((early, regions * ghost), bf16),
        ],
        in_specs=[SMEM] + [VMEM] * 3,
        out_specs=[VMEM] * 5,
        compiler_params=params(20),
        cost_estimate=cost(table_flops * owned * 8),
        name="gather_owned",
    )(cell_count, index, weight, flipped)

    out, *ret = pl.pallas_call(
        functools.partial(element_kernel, width, pairs, owned),
        out_shape=[jax.ShapeDtypeStruct((channels, elements), bf16)] + list_shape,
        in_specs=[VMEM] * (8 + regions),
        out_specs=[VMEM] * (1 + regions),
        scratch_shapes=[
            pltpu.VMEM((regions * ghost, channels), bf16),
            pltpu.VMEM((2 * channels, elements), bf16),
            pltpu.VMEM((max(elements - early, PACK), regions * ghost), bf16),
            pltpu.VMEM((regions * ghost, channels), f32),
        ],
        compiler_params=params(24),
        cost_estimate=cost(table_flops * regions * ghost * 2),
        name="elements",
    )(visc, ein, column, share, table, turned, mats_v, mats_p, *got)
    back = [exchange(block, *pair) for block, pair in zip(ret, pairs)]

    part, *hits = pl.pallas_call(
        functools.partial(scatter_kernel, width),
        out_shape=[jax.ShapeDtypeStruct((owned, channels), f32)] + [jax.ShapeDtypeStruct((owned, ghost), bf16)] * regions,
        in_specs=[VMEM] * 4,
        out_specs=[VMEM] * (1 + regions),
        scratch_shapes=[pltpu.VMEM((elements, owned), bf16)],
        compiler_params=params(24),
        cost_estimate=cost(table_flops * owned * 8),
        name="scatter_owned",
    )(column, share, out, names)

    return pl.pallas_call(
        functools.partial(finish_kernel, regions),
        out_shape=jax.ShapeDtypeStruct((owned, channels), f32),
        in_specs=[VMEM] * (1 + 2 * regions),
        out_specs=VMEM,
        compiler_params=params(16),
        cost_estimate=cost(2 * owned * channels * regions * ghost),
        name="finish",
    )(part, *hits, *back)


def solution(mesh):
    return jax.shard_map(
        per_device,
        mesh=mesh,
        in_specs=(
            P(AXES, None),
            P(AXES),
            P(AXES, None),
            P(AXES, None),
            P(AXES, None, None),
            P(AXES, None),
            P(AXES),
            P(),
            P(),
        ),
        out_specs=P(AXES, None),
        check_vma=False,
    )
```

```python
import functools

import jax
import jax.numpy as jnp
from jax import lax
from jax.experimental import pallas as pl
from jax.experimental.pallas import tpu as pltpu
from jax.sharding import PartitionSpec as P

AXES = ("curve", "seg")
PACK = 16
TILE = 256
VMEM = pl.BlockSpec(memory_space=pltpu.VMEM)
SMEM = pl.BlockSpec(memory_space=pltpu.SMEM)
HBM = pl.BlockSpec(memory_space=pltpu.HBM)


def matchings(region_count):
    reaches = range(1, region_count // 2 + 1)
    return [(reach, 1) for reach in reaches] + [(reach, 0) for reach in reversed(reaches)]


def exchange(block, distance, parity):
    total = lax.axis_size(AXES)
    swaps = [(d, d + distance) for d in range(total - distance) if (d // distance) % 2 == parity]
    left = sorted(set(range(total)) - {d for swap in swaps for d in swap})
    swaps += list(zip(left[::2], left[1::2]))
    return lax.ppermute(block, AXES, swaps + [(b, a) for a, b in swaps])


def send_region(distance, parity):
    seg = lax.axis_size("seg")
    me = lax.axis_index("curve") * seg + lax.axis_index("seg")
    down = (lax.div(me, distance) + parity) % 2
    there = me + distance * (1 - 2 * down)
    return 2 * (distance - 1) + down, (there >= 0) & (there < seg * lax.axis_size("curve"))


def transposed(values):
    return values.astype(jnp.float32).T.astype(jnp.bfloat16)


def matmul(a, b):
    return jnp.dot(a, b, preferred_element_type=jnp.float32)


def matmul_nt(a, b):
    return lax.dot_general(a, b, (((1,), (1,)), ((), ())), preferred_element_type=jnp.float32)


def one_hot(names, rows):
    wide = jnp.broadcast_to(names, (PACK, names.shape[1])).astype(jnp.int16)
    iota = lax.broadcasted_iota(jnp.int32, wide.shape, 0)
    one, zero = jnp.ones(wide.shape, jnp.bfloat16), jnp.zeros(wide.shape, jnp.bfloat16)
    return jnp.concatenate([jnp.where(wide == (iota + g * PACK).astype(jnp.int16), one, zero) for g in range(rows // PACK)], axis=0)


def select_kernel(pairs, loads, mirror_hbm, live_hbm, sol_hbm, *rest):
    n = len(pairs)
    load_refs, rest = rest[:loads], rest[loads:]
    sent_refs, (names_ref, flipped_ref), rest = rest[:n], rest[n : n + 2], rest[n + 2 :]
    copy_refs, (mirror_ref, live_ref, sol_ref, sems) = rest[:loads], rest[loads:]
    first = [
        pltpu.make_async_copy(src, dst, sems.at[i])
        for i, (src, dst) in enumerate(((sol_hbm, sol_ref), (mirror_hbm, mirror_ref), (live_hbm, live_ref)))
    ]
    later = [pltpu.make_async_copy(src, dst, sems.at[len(first) + i]) for i, (src, dst) in enumerate(zip(load_refs, copy_refs))]
    for copy in first + later:
        copy.start()
    for copy in first:
        copy.wait()
    rows, ghost = sol_ref.shape[0], mirror_ref.shape[2]
    flipped = transposed(sol_ref[...])
    flipped_ref[...] = flipped
    lane = lax.broadcasted_iota(jnp.int32, (1, ghost), 1)
    for m, (distance, parity) in enumerate(pairs):
        region, there = send_region(distance, parity)
        names = jnp.where(lane < jnp.where(there, live_ref[0, region], 0), mirror_ref[0, pl.ds(region, 1), :], -1)
        names_ref[pl.ds(m, 1), :] = names
        sent_refs[m][...] = matmul(flipped, one_hot(names, rows)).T.astype(jnp.bfloat16)
    for copy in later:
        copy.wait()


def slot_rows(index_ref, weight_ref, count, lanes):
    slots, width = index_ref.shape[0], lanes.size
    live = lax.broadcasted_iota(jnp.int32, (1, width), 1) + lanes.start < count
    names = [index_ref[pl.ds(i, 1), lanes] for i in range(slots)]
    codes = [weight_ref[pl.ds(i, 1), lanes] for i in range(slots)]
    sums = list(codes)
    for i in range(slots):
        for j in range(i + 1, slots):
            sums[i] = sums[i] + jnp.where(names[i] == names[j], codes[j], 0)
    out = []
    for i in range(slots):
        scaled = jnp.where(live, sums[i].astype(jnp.float32) * 0.125, 0.0)
        column = jnp.broadcast_to(names[i], (PACK, width)).astype(jnp.int16)
        weight = jnp.broadcast_to(scaled, (PACK, width)).astype(jnp.bfloat16)
        out.append((column, weight))
    return out


def load_rows(column_ref, share_ref, lanes, first):
    slots = column_ref.shape[0] // PACK
    return [(column_ref[i * PACK : (i + 1) * PACK, lanes], share_ref[i * PACK : (i + 1) * PACK, lanes]) for i in range(first, slots)]


def selection(slots, base, rows):
    shape = slots[0][0].shape
    iota = lax.broadcasted_iota(jnp.int32, shape, 0)
    pieces = []
    for g in range(rows // PACK):
        here = (iota + (base + g * PACK)).astype(jnp.int16)
        piece = jnp.zeros(shape, jnp.bfloat16)
        for column, weight in reversed(slots):
            piece = jnp.where(column == here, weight, piece)
        pieces.append(piece)
    return jnp.concatenate(pieces, axis=0)


def spans(total, width):
    return [pl.ds(start, min(width, total - start)) for start in range(0, total, width)]


def by_load(count, total, work):
    few = total // 4
    if few % TILE:
        return work(total)
    pl.when(count <= few)(functools.partial(work, few))
    pl.when(count > few)(functools.partial(work, total))


def gather_kernel(width, early, count_ref, index_ref, weight_ref, flipped_ref, ein_ref, column_ref, share_ref, table_ref, turned_ref):
    owned, columns = flipped_ref.shape[1], table_ref.shape[0]

    def work(total):
        for lanes in spans(total, width):
            slots = slot_rows(index_ref, weight_ref, count_ref[0], lanes)
            for i, (column, share) in enumerate(slots):
                column_ref[i * PACK : (i + 1) * PACK, lanes] = column
                share_ref[i * PACK : (i + 1) * PACK, lanes] = share
            ein_ref[:, lanes] = sum(matmul(flipped_ref[:, rows], selection(slots, rows.start, rows.size)) for rows in spans(owned, TILE))
            if lanes.start < early:
                for rows in spans(columns, TILE):
                    table = selection(slots[1:], owned + rows.start, rows.size)
                    table_ref[rows, lanes] = table
                    turned_ref[lanes, rows] = table.T

    by_load(count_ref[0], ein_ref.shape[1], work)


def element_kernel(
    width, early, pairs, owned, count_ref, visc_ref, ein_ref, column_ref, share_ref, table_ref, turned_ref, mats_v_ref, mats_p_ref, *rest
):
    n = len(pairs)
    ghost_refs, out_ref, ret_refs, rest = rest[:n], rest[n], rest[n + 1 : 2 * n + 1], rest[2 * n + 1 :]
    ghost_all, stacked_ref, late_ref, back = rest
    ghost, channels = ghost_refs[0].shape
    columns = table_ref.shape[0]
    spots = []
    for (distance, parity), ghost_ref in zip(pairs, ghost_refs):
        sent, _ = send_region(distance, parity)
        got = 4 * (distance - 1) + 1 - sent
        spot = pl.ds(pl.multiple_of(got * ghost, PACK), ghost)
        spots.append(spot)
        ghost_all[spot, :] = ghost_ref[...]

    def work(total):
        flipped = transposed(ghost_all[...])
        both = jnp.concatenate([mats_v_ref[...].astype(jnp.float32).T, mats_p_ref[...].astype(jnp.float32).T], axis=1).astype(jnp.bfloat16)
        blocks = spans(total, width)
        for lanes in blocks:
            ein = ein_ref[:, lanes]
            if lanes.start < early:
                ein = ein + matmul(flipped, table_ref[:, lanes])
            else:
                slots = load_rows(column_ref, share_ref, lanes, 1)
                for rows in spans(columns, TILE):
                    table = selection(slots, owned + rows.start, rows.size)
                    late_ref[pl.ds(lanes.start - early, width), rows] = table.T
                    ein = ein + matmul(flipped[:, rows.start : rows.start + rows.size], table)
            stacked_ref[:channels, lanes] = (ein * visc_ref[:, lanes]).astype(jnp.bfloat16)
            stacked_ref[channels:, lanes] = ein.astype(jnp.bfloat16)
        for lanes in blocks:
            out_ref[:, lanes] = matmul(both, stacked_ref[:, lanes]).astype(jnp.bfloat16)
        first = min(early, total)
        summed = matmul(out_ref[:, :first], turned_ref[:first, :])
        if total > early:
            summed = summed + matmul(out_ref[:, early:total], late_ref[: total - early, :])
        back[...] = summed.T
        for spot, ret_ref in zip(spots, ret_refs):
            ret_ref[...] = back[spot, :].astype(jnp.bfloat16)

    by_load(count_ref[0], ein_ref.shape[1], work)


def scatter_kernel(width, count_ref, column_ref, share_ref, out_ref, names_ref, part_ref, *rest):
    hit_refs, turned_ref = rest[:-1], rest[-1]
    owned = part_ref.shape[0]

    def work(total):
        for lanes in spans(total, width):
            slots = load_rows(column_ref, share_ref, lanes, 0)
            for rows in spans(owned, TILE):
                turned_ref[lanes, rows] = selection(slots, rows.start, rows.size).T
        part_ref[...] = matmul(out_ref[:, :total], turned_ref[:total, :]).T

    by_load(count_ref[0], out_ref.shape[1], work)
    for m, hit_ref in enumerate(hit_refs):
        hit_ref[...] = one_hot(names_ref[pl.ds(m, 1), :], owned)


def finish_kernel(n, part_ref, *rest):
    hit_refs, back_refs, res_ref = rest[:n], rest[n : 2 * n], rest[2 * n]
    total = part_ref[...]
    for hit_ref, back_ref in zip(hit_refs, back_refs):
        total = total + matmul(hit_ref[...], back_ref[...])
    res_ref[...] = total


def params(limit):
    return pltpu.CompilerParams(vmem_limit_bytes=limit * 1024 * 1024)


def cost(flops):
    return pl.CostEstimate(flops=flops, bytes_accessed=1 << 20, transcendentals=0)


def like(*arrays):
    return [jax.ShapeDtypeStruct(a.shape, a.dtype) for a in arrays]


def per_device(
    solution,
    viscosity,
    slot_index,
    slot_weight,
    mirror_rows,
    ghost_live,
    cell_count,
    viscous_block,
    pressure_block,
):
    owned, channels = solution.shape
    regions, ghost = mirror_rows.shape[1:]
    elements = viscosity.shape[0]
    width = min(TILE, elements)
    early = elements // 2
    slots = slot_index.shape[1]
    pairs = matchings(regions)
    bf16, f32 = jnp.bfloat16, jnp.float32
    table_flops = 2 * elements * channels
    list_shape = [jax.ShapeDtypeStruct((ghost, channels), bf16)] * regions
    loads = [slot_index.T, slot_weight.T, viscosity.reshape(1, elements), viscous_block, pressure_block]

    outs = pl.pallas_call(
        functools.partial(select_kernel, pairs, len(loads)),
        out_shape=list_shape
        + [
            jax.ShapeDtypeStruct((regions, ghost), jnp.int32),
            jax.ShapeDtypeStruct((channels, owned), bf16),
        ]
        + like(*loads),
        in_specs=[HBM] * (3 + len(loads)),
        out_specs=[VMEM] * (regions + 2 + len(loads)),
        scratch_shapes=[
            pltpu.VMEM(mirror_rows.shape, jnp.int32),
            pltpu.SMEM(ghost_live.shape, jnp.int32),
            pltpu.VMEM(solution.shape, bf16),
            pltpu.SemaphoreType.DMA((3 + len(loads),)),
        ],
        compiler_params=params(16),
        cost_estimate=cost(2 * owned * channels * regions * ghost),
        name="select",
    )(*[pltpu.with_memory_space_constraint(a, pltpu.HBM) for a in (mirror_rows, ghost_live, solution, *loads)])
    sent, (names, flipped, index, weight, visc, mats_v, mats_p) = outs[:regions], outs[regions:]
    got = [exchange(block, *pair) for block, pair in zip(sent, pairs)]

    ein, column, share, table, turned = pl.pallas_call(
        functools.partial(gather_kernel, width, early),
        out_shape=[
            jax.ShapeDtypeStruct((channels, elements), f32),
            jax.ShapeDtypeStruct((PACK * slots, elements), jnp.int16),
            jax.ShapeDtypeStruct((PACK * slots, elements), bf16),
            jax.ShapeDtypeStruct((regions * ghost, early), bf16),
            jax.ShapeDtypeStruct((early, regions * ghost), bf16),
        ],
        in_specs=[SMEM] + [VMEM] * 3,
        out_specs=[VMEM] * 5,
        compiler_params=params(20),
        cost_estimate=cost(table_flops * owned * 8),
        name="gather_owned",
    )(cell_count, index, weight, flipped)

    out, *ret = pl.pallas_call(
        functools.partial(element_kernel, width, early, pairs, owned),
        out_shape=[jax.ShapeDtypeStruct((channels, elements), bf16)] + list_shape,
        in_specs=[SMEM] + [VMEM] * (8 + regions),
        out_specs=[VMEM] * (1 + regions),
        scratch_shapes=[
            pltpu.VMEM((regions * ghost, channels), bf16),
            pltpu.VMEM((2 * channels, elements), bf16),
            pltpu.VMEM((max(elements - early, PACK), regions * ghost), bf16),
            pltpu.VMEM((regions * ghost, channels), f32),
        ],
        compiler_params=params(24),
        cost_estimate=cost(table_flops * regions * ghost * 2),
        name="elements",
    )(cell_count, visc, ein, column, share, table, turned, mats_v, mats_p, *got)
    back = [exchange(block, *pair) for block, pair in zip(ret, pairs)]

    part, *hits = pl.pallas_call(
        functools.partial(scatter_kernel, width),
        out_shape=[jax.ShapeDtypeStruct((owned, channels), f32)] + [jax.ShapeDtypeStruct((owned, ghost), bf16)] * regions,
        in_specs=[SMEM] + [VMEM] * 4,
        out_specs=[VMEM] * (1 + regions),
        scratch_shapes=[pltpu.VMEM((elements, owned), bf16)],
        compiler_params=params(24),
        cost_estimate=cost(table_flops * owned * 8),
        name="scatter_owned",
    )(cell_count, column, share, out, names)

    return pl.pallas_call(
        functools.partial(finish_kernel, regions),
        out_shape=jax.ShapeDtypeStruct((owned, channels), f32),
        in_specs=[VMEM] * (1 + 2 * regions),
        out_specs=VMEM,
        compiler_params=params(16),
        cost_estimate=cost(2 * owned * channels * regions * ghost),
        name="finish",
    )(part, *hits, *back)


def solution(mesh):
    return jax.shard_map(
        per_device,
        mesh=mesh,
        in_specs=(
            P(AXES, None),
            P(AXES),
            P(AXES, None),
            P(AXES, None),
            P(AXES, None, None),
            P(AXES, None),
            P(AXES),
            P(),
            P(),
        ),
        out_specs=P(AXES, None),
        check_vma=False,
    )
```

```python
import functools

import jax
import jax.numpy as jnp
from jax import lax
from jax.experimental import pallas as pl
from jax.experimental.pallas import tpu as pltpu
from jax.sharding import PartitionSpec as P


AXES = ("curve", "seg")
PACK = 16
TILE = 256
VMEM = pl.BlockSpec(memory_space=pltpu.VMEM)
SMEM = pl.BlockSpec(memory_space=pltpu.SMEM)
HBM = pl.BlockSpec(memory_space=pltpu.HBM)


def matchings(region_count):
    reaches = range(1, region_count // 2 + 1)
    return [(reach, 1) for reach in reaches] + [(reach, 0) for reach in reversed(reaches)]


def both_ways(swaps):
    return swaps + [(b, a) for a, b in swaps]


def ring(*devices):
    return list(zip(devices, devices[1:] + devices[:1]))


def exchange(blocks, pairs):
    n = lax.axis_size(AXES)
    routes = []
    for distance, parity in pairs:
        swaps = [(d, d + distance) for d in range(n - distance) if (d // distance) % 2 == parity]
        left = sorted(set(range(n)) - {d for swap in swaps for d in swap})
        if left == [0, n - 1]:
            detour = ring(2, 1, 0, 3) + both_ways([(d, d + 1) for d in range(4, n - 4, 2)]) + ring(n - 3, n - 2, n - 1, n - 4)
            routes.append(ring(0, 1, 2) + both_ways(swaps[1:-1]) + ring(n - 1, n - 2, n - 3))
            source = len(routes) - 1
        else:
            routes.append(both_ways(swaps + list(zip(left[::2], left[1::2]))))
    routes.append(detour)
    got = []
    for block, route in zip([*blocks, blocks[source]], routes):
        got.append(lax.ppermute(block, AXES, route))
    return got


def position():
    return lax.axis_index("curve") * lax.axis_size("seg") + lax.axis_index("seg"), lax.axis_size("curve") * lax.axis_size("seg")


def received(pairs, refs):
    me, total = position()
    detoured = (me == 1) | (me == total - 2)
    out = []
    for (distance, parity), ref in zip(pairs, refs):
        value = ref[...]
        if (distance, parity) == (1, 1):
            value = jnp.where(detoured, refs[-1][...], value)
            value = jnp.where((me == 0) | (me == total - 1), jnp.zeros_like(value), value)
        out.append(value)
    return out


def send_region(distance, parity):
    me, total = position()
    down = (lax.div(me, distance) + parity) % 2
    there = me + distance * (1 - 2 * down)
    return 2 * (distance - 1) + down, (there >= 0) & (there < total)


def transposed(values):
    return values.astype(jnp.float32).T.astype(jnp.bfloat16)


def matmul(a, b):
    return jnp.dot(a, b, preferred_element_type=jnp.float32)


def one_hot(names, rows):
    wide = jnp.broadcast_to(names, (PACK, names.shape[1])).astype(jnp.int16)
    iota = lax.broadcasted_iota(jnp.int32, wide.shape, 0)
    one, zero = jnp.ones(wide.shape, jnp.bfloat16), jnp.zeros(wide.shape, jnp.bfloat16)
    return jnp.concatenate([jnp.where(wide == (iota + g * PACK).astype(jnp.int16), one, zero) for g in range(rows // PACK)], axis=0)


def select_kernel(pairs, loads, mirror_hbm, live_hbm, sol_hbm, *rest):
    n = len(pairs)
    load_refs, rest = rest[:loads], rest[loads:]
    sent_refs, (names_ref, flipped_ref), rest = rest[:n], rest[n : n + 2], rest[n + 2 :]
    copy_refs, (mirror_ref, live_ref, sol_ref, sems) = rest[:loads], rest[loads:]
    first = [
        pltpu.make_async_copy(src, dst, sems.at[i])
        for i, (src, dst) in enumerate(((sol_hbm, sol_ref), (mirror_hbm, mirror_ref), (live_hbm, live_ref)))
    ]
    later = [pltpu.make_async_copy(src, dst, sems.at[len(first) + i]) for i, (src, dst) in enumerate(zip(load_refs, copy_refs))]
    for copy in first + later:
        copy.start()
    for copy in first:
        copy.wait()
    rows, ghost = sol_ref.shape[0], mirror_ref.shape[2]
    flipped = transposed(sol_ref[...])
    flipped_ref[...] = flipped
    lane = lax.broadcasted_iota(jnp.int32, (1, ghost), 1)
    for m, (distance, parity) in enumerate(pairs):
        region, there = send_region(distance, parity)
        names = jnp.where(lane < jnp.where(there, live_ref[0, region], 0), mirror_ref[0, pl.ds(region, 1), :], -1)
        names_ref[pl.ds(m, 1), :] = names
        sent_refs[m][...] = matmul(flipped, one_hot(names, rows)).T.astype(jnp.bfloat16)
    for copy in later:
        copy.wait()


def slot_rows(index_ref, weight_ref, count, lanes):
    slots, width = index_ref.shape[0], lanes.size
    live = lax.broadcasted_iota(jnp.int32, (1, width), 1) + lanes.start < count
    names = [index_ref[pl.ds(i, 1), lanes] for i in range(slots)]
    codes = [weight_ref[pl.ds(i, 1), lanes] for i in range(slots)]
    sums = list(codes)
    for i in range(slots):
        for j in range(i + 1, slots):
            sums[i] = sums[i] + jnp.where(names[i] == names[j], codes[j], 0)
    out = []
    for i in range(slots):
        scaled = jnp.where(live, sums[i].astype(jnp.float32) * 0.125, 0.0)
        column = jnp.broadcast_to(names[i], (PACK, width)).astype(jnp.int16)
        weight = jnp.broadcast_to(scaled, (PACK, width)).astype(jnp.bfloat16)
        out.append((column, weight))
    return out


def load_rows(column_ref, share_ref, lanes, first):
    slots = column_ref.shape[0] // PACK
    return [(column_ref[i * PACK : (i + 1) * PACK, lanes], share_ref[i * PACK : (i + 1) * PACK, lanes]) for i in range(first, slots)]


def selection(slots, base, rows):
    shape = slots[0][0].shape
    iota = lax.broadcasted_iota(jnp.int32, shape, 0)
    pieces = []
    for g in range(rows // PACK):
        here = (iota + (base + g * PACK)).astype(jnp.int16)
        piece = jnp.zeros(shape, jnp.bfloat16)
        for column, weight in reversed(slots):
            piece = jnp.where(column == here, weight, piece)
        pieces.append(piece)
    return jnp.concatenate(pieces, axis=0)


def spans(total, width):
    return [pl.ds(start, min(width, total - start)) for start in range(0, total, width)]


def by_load(count, total, work):
    few = total // 4
    if few % TILE:
        return work(total)
    pl.when(count <= few)(functools.partial(work, few))
    pl.when(count > few)(functools.partial(work, total))


def gather_kernel(width, early, count_ref, index_ref, weight_ref, flipped_ref, ein_ref, column_ref, share_ref, table_ref, turned_ref):
    owned, columns = flipped_ref.shape[1], table_ref.shape[0]

    def work(total):
        for lanes in spans(total, width):
            slots = slot_rows(index_ref, weight_ref, count_ref[0], lanes)
            for i, (column, share) in enumerate(slots):
                column_ref[i * PACK : (i + 1) * PACK, lanes] = column
                share_ref[i * PACK : (i + 1) * PACK, lanes] = share
            ein_ref[:, lanes] = sum(matmul(flipped_ref[:, rows], selection(slots, rows.start, rows.size)) for rows in spans(owned, TILE))
            if lanes.start < early:
                for rows in spans(columns, TILE):
                    table = selection(slots[1:], owned + rows.start, rows.size)
                    table_ref[rows, lanes] = table
                    turned_ref[lanes, rows] = table.T

    by_load(count_ref[0], ein_ref.shape[1], work)


def element_kernel(
    width, early, pairs, owned, count_ref, visc_ref, ein_ref, column_ref, share_ref, table_ref, turned_ref, mats_v_ref, mats_p_ref, *rest
):
    n = len(pairs)
    ghost_refs, out_ref, ret_refs, rest = rest[: n + 1], rest[n + 1], rest[n + 2 : 2 * n + 2], rest[2 * n + 2 :]
    ghost_all, stacked_ref, late_ref, back = rest
    ghost, channels = ghost_refs[0].shape
    columns = table_ref.shape[0]
    spots = []
    for (distance, parity), arrived in zip(pairs, received(pairs, ghost_refs)):
        sent, _ = send_region(distance, parity)
        got = 4 * (distance - 1) + 1 - sent
        spot = pl.ds(pl.multiple_of(got * ghost, PACK), ghost)
        spots.append(spot)
        ghost_all[spot, :] = arrived

    def work(total):
        flipped = transposed(ghost_all[...])
        both = jnp.concatenate([mats_v_ref[...].astype(jnp.float32).T, mats_p_ref[...].astype(jnp.float32).T], axis=1).astype(jnp.bfloat16)
        blocks = spans(total, width)
        for lanes in blocks:
            ein = ein_ref[:, lanes]
            if lanes.start < early:
                ein = ein + matmul(flipped, table_ref[:, lanes])
            else:
                slots = load_rows(column_ref, share_ref, lanes, 1)
                for rows in spans(columns, TILE):
                    table = selection(slots, owned + rows.start, rows.size)
                    late_ref[pl.ds(lanes.start - early, width), rows] = table.T
                    ein = ein + matmul(flipped[:, rows.start : rows.start + rows.size], table)
            stacked_ref[:channels, lanes] = (ein * visc_ref[:, lanes]).astype(jnp.bfloat16)
            stacked_ref[channels:, lanes] = ein.astype(jnp.bfloat16)
        for lanes in blocks:
            out_ref[:, lanes] = matmul(both, stacked_ref[:, lanes]).astype(jnp.bfloat16)
        first = min(early, total)
        summed = matmul(out_ref[:, :first], turned_ref[:first, :])
        if total > early:
            summed = summed + matmul(out_ref[:, early:total], late_ref[: total - early, :])
        back[...] = summed.T
        for spot, ret_ref in zip(spots, ret_refs):
            ret_ref[...] = back[spot, :].astype(jnp.bfloat16)

    by_load(count_ref[0], ein_ref.shape[1], work)


def scatter_kernel(width, count_ref, column_ref, share_ref, out_ref, names_ref, part_ref, *rest):
    hit_refs, turned_ref = rest[:-1], rest[-1]
    owned = part_ref.shape[0]

    def work(total):
        for lanes in spans(total, width):
            slots = load_rows(column_ref, share_ref, lanes, 0)
            for rows in spans(owned, TILE):
                turned_ref[lanes, rows] = selection(slots, rows.start, rows.size).T
        part_ref[...] = matmul(out_ref[:, :total], turned_ref[:total, :]).T

    by_load(count_ref[0], out_ref.shape[1], work)
    for m, hit_ref in enumerate(hit_refs):
        hit_ref[...] = one_hot(names_ref[pl.ds(m, 1), :], owned)


def finish_kernel(pairs, part_ref, *rest):
    n = len(pairs)
    hit_refs, back_refs, res_ref = rest[:n], rest[n : 2 * n + 1], rest[2 * n + 1]
    total = part_ref[...]
    for hit_ref, arrived in zip(hit_refs, received(pairs, back_refs)):
        total = total + matmul(hit_ref[...], arrived)
    res_ref[...] = total


def params(limit):
    return pltpu.CompilerParams(vmem_limit_bytes=limit * 1024 * 1024)


def cost(flops):
    return pl.CostEstimate(flops=flops, bytes_accessed=1 << 20, transcendentals=0)


def like(*arrays):
    return [jax.ShapeDtypeStruct(a.shape, a.dtype) for a in arrays]


def per_device(
    solution,
    viscosity,
    slot_index,
    slot_weight,
    mirror_rows,
    ghost_live,
    cell_count,
    viscous_block,
    pressure_block,
):
    owned, channels = solution.shape
    regions, ghost = mirror_rows.shape[1:]
    elements = viscosity.shape[0]
    width = min(TILE, elements)
    early = elements // 2
    slots = slot_index.shape[1]
    pairs = matchings(regions)
    bf16, f32 = jnp.bfloat16, jnp.float32
    table_flops = 2 * elements * channels
    list_shape = [jax.ShapeDtypeStruct((ghost, channels), bf16)] * regions
    loads = [slot_index.T, slot_weight.T, viscosity.reshape(1, elements), viscous_block, pressure_block]

    outs = pl.pallas_call(
        functools.partial(select_kernel, pairs, len(loads)),
        out_shape=list_shape
        + [
            jax.ShapeDtypeStruct((regions, ghost), jnp.int32),
            jax.ShapeDtypeStruct((channels, owned), bf16),
        ]
        + like(*loads),
        in_specs=[HBM] * (3 + len(loads)),
        out_specs=[VMEM] * (regions + 2 + len(loads)),
        scratch_shapes=[
            pltpu.VMEM(mirror_rows.shape, jnp.int32),
            pltpu.SMEM(ghost_live.shape, jnp.int32),
            pltpu.VMEM(solution.shape, bf16),
            pltpu.SemaphoreType.DMA((3 + len(loads),)),
        ],
        compiler_params=params(16),
        cost_estimate=cost(2 * owned * channels * regions * ghost),
        name="select",
    )(*[pltpu.with_memory_space_constraint(a, pltpu.HBM) for a in (mirror_rows, ghost_live, solution, *loads)])
    sent, (names, flipped, index, weight, visc, mats_v, mats_p) = outs[:regions], outs[regions:]
    got = exchange(sent, pairs)

    ein, column, share, table, turned = pl.pallas_call(
        functools.partial(gather_kernel, width, early),
        out_shape=[
            jax.ShapeDtypeStruct((channels, elements), f32),
            jax.ShapeDtypeStruct((PACK * slots, elements), jnp.int16),
            jax.ShapeDtypeStruct((PACK * slots, elements), bf16),
            jax.ShapeDtypeStruct((regions * ghost, early), bf16),
            jax.ShapeDtypeStruct((early, regions * ghost), bf16),
        ],
        in_specs=[SMEM] + [VMEM] * 3,
        out_specs=[VMEM] * 5,
        compiler_params=params(20),
        cost_estimate=cost(table_flops * owned * 8),
        name="gather_owned",
    )(cell_count, index, weight, flipped)

    out, *ret = pl.pallas_call(
        functools.partial(element_kernel, width, early, pairs, owned),
        out_shape=[jax.ShapeDtypeStruct((channels, elements), bf16)] + list_shape,
        in_specs=[SMEM] + [VMEM] * (9 + regions),
        out_specs=[VMEM] * (1 + regions),
        scratch_shapes=[
            pltpu.VMEM((regions * ghost, channels), bf16),
            pltpu.VMEM((2 * channels, elements), bf16),
            pltpu.VMEM((max(elements - early, PACK), regions * ghost), bf16),
            pltpu.VMEM((regions * ghost, channels), f32),
        ],
        compiler_params=params(24),
        cost_estimate=cost(table_flops * regions * ghost * 2),
        name="elements",
    )(cell_count, visc, ein, column, share, table, turned, mats_v, mats_p, *got)
    back = exchange(ret, pairs)

    part, *hits = pl.pallas_call(
        functools.partial(scatter_kernel, width),
        out_shape=[jax.ShapeDtypeStruct((owned, channels), f32)] + [jax.ShapeDtypeStruct((owned, ghost), bf16)] * regions,
        in_specs=[SMEM] + [VMEM] * 4,
        out_specs=[VMEM] * (1 + regions),
        scratch_shapes=[pltpu.VMEM((elements, owned), bf16)],
        compiler_params=params(24),
        cost_estimate=cost(table_flops * owned * 8),
        name="scatter_owned",
    )(cell_count, column, share, out, names)

    return pl.pallas_call(
        functools.partial(finish_kernel, pairs),
        out_shape=jax.ShapeDtypeStruct((owned, channels), f32),
        in_specs=[VMEM] * (2 + 2 * regions),
        out_specs=VMEM,
        compiler_params=params(16),
        cost_estimate=cost(2 * owned * channels * regions * ghost),
        name="finish",
    )(part, *hits, *back)


def solution(mesh):
    return jax.shard_map(
        per_device,
        mesh=mesh,
        in_specs=(
            P(AXES, None),
            P(AXES),
            P(AXES, None),
            P(AXES, None),
            P(AXES, None, None),
            P(AXES, None),
            P(AXES),
            P(),
            P(),
        ),
        out_specs=P(AXES, None),
        check_vma=False,
    )
```

```python
import functools

import jax
import jax.numpy as jnp
from jax import lax
from jax.experimental import pallas as pl
from jax.experimental.pallas import tpu as pltpu
from jax.sharding import PartitionSpec as P


AXES = ("curve", "seg")
PACK = 16
TILE = 256
VMEM = pl.BlockSpec(memory_space=pltpu.VMEM)
SMEM = pl.BlockSpec(memory_space=pltpu.SMEM)
HBM = pl.BlockSpec(memory_space=pltpu.HBM)


def matchings(region_count):
    reaches = range(1, region_count // 2 + 1)
    return [(reach, 1) for reach in reaches] + [(reach, 0) for reach in reversed(reaches)]


def both_ways(swaps):
    return swaps + [(b, a) for a, b in swaps]


def ring(*devices):
    return list(zip(devices, devices[1:] + devices[:1]))


def exchange(blocks, pairs):
    n = lax.axis_size(AXES)
    routes = []
    for distance, parity in pairs:
        swaps = [(d, d + distance) for d in range(n - distance) if (d // distance) % 2 == parity]
        left = sorted(set(range(n)) - {d for swap in swaps for d in swap})
        if left == [0, n - 1]:
            detour = ring(2, 1, 0, 3) + both_ways([(d, d + 1) for d in range(4, n - 4, 2)]) + ring(n - 3, n - 2, n - 1, n - 4)
            routes.append(ring(0, 1, 2) + both_ways(swaps[1:-1]) + ring(n - 1, n - 2, n - 3))
            source = len(routes) - 1
        else:
            routes.append(both_ways(swaps + list(zip(left[::2], left[1::2]))))
    routes.append(detour)
    got = []
    for block, route in zip([*blocks, blocks[source]], routes):
        got.append(lax.ppermute(block, AXES, route))
    return got


def position():
    return lax.axis_index("curve") * lax.axis_size("seg") + lax.axis_index("seg"), lax.axis_size("curve") * lax.axis_size("seg")


def received(pairs, refs):
    me, total = position()
    detoured = (me == 1) | (me == total - 2)
    out = []
    for (distance, parity), ref in zip(pairs, refs):
        value = ref[...]
        if (distance, parity) == (1, 1):
            value = jnp.where(detoured, refs[-1][...], value)
            value = jnp.where((me == 0) | (me == total - 1), jnp.zeros_like(value), value)
        out.append(value)
    return out


def send_region(distance, parity):
    me, total = position()
    down = (lax.div(me, distance) + parity) % 2
    there = me + distance * (1 - 2 * down)
    return 2 * (distance - 1) + down, (there >= 0) & (there < total)


def transposed(values):
    return values.astype(jnp.bfloat16).T


def matmul(a, b):
    return jnp.dot(a, b, preferred_element_type=jnp.float32)


def one_hot(names, rows):
    wide = jnp.broadcast_to(names, (PACK, names.shape[1])).astype(jnp.int16)
    iota = lax.broadcasted_iota(jnp.int32, wide.shape, 0)
    one, zero = jnp.ones(wide.shape, jnp.bfloat16), jnp.zeros(wide.shape, jnp.bfloat16)
    return jnp.concatenate([jnp.where(wide == (iota + g * PACK).astype(jnp.int16), one, zero) for g in range(rows // PACK)], axis=0)


def select_kernel(pairs, loads, mirror_hbm, live_hbm, sol_hbm, *rest):
    n = len(pairs)
    load_refs, rest = rest[:loads], rest[loads:]
    sent_refs, (names_ref, flipped_ref), rest = rest[:n], rest[n : n + 2], rest[n + 2 :]
    copy_refs, (mirror_ref, live_ref, sol_ref, sems) = rest[:loads], rest[loads:]
    first = [
        pltpu.make_async_copy(src, dst, sems.at[i])
        for i, (src, dst) in enumerate(((sol_hbm, sol_ref), (mirror_hbm, mirror_ref), (live_hbm, live_ref)))
    ]
    later = [pltpu.make_async_copy(src, dst, sems.at[len(first) + i]) for i, (src, dst) in enumerate(zip(load_refs, copy_refs))]
    for copy in first + later:
        copy.start()
    for copy in first:
        copy.wait()
    rows, ghost = sol_ref.shape[0], mirror_ref.shape[2]
    flipped = transposed(sol_ref[...])
    flipped_ref[...] = flipped
    lane = lax.broadcasted_iota(jnp.int32, (1, ghost), 1)
    for m, (distance, parity) in enumerate(pairs):
        region, there = send_region(distance, parity)
        names = jnp.where(lane < jnp.where(there, live_ref[0, region], 0), mirror_ref[0, pl.ds(region, 1), :], -1)
        names_ref[pl.ds(m, 1), :] = names
        sent_refs[m][...] = transposed(matmul(flipped, one_hot(names, rows)))
    for copy in later:
        copy.wait()


def slot_rows(index_ref, weight_ref, count, lanes):
    slots, width = index_ref.shape[0], lanes.size
    live = lax.broadcasted_iota(jnp.int32, (1, width), 1) + lanes.start < count
    names = [index_ref[pl.ds(i, 1), lanes] for i in range(slots)]
    codes = [weight_ref[pl.ds(i, 1), lanes] for i in range(slots)]
    sums = list(codes)
    for i in range(slots):
        for j in range(i + 1, slots):
            sums[i] = sums[i] + jnp.where(names[i] == names[j], codes[j], 0)
    out = []
    for i in range(slots):
        scaled = jnp.where(live, sums[i].astype(jnp.float32) * 0.125, 0.0)
        column = jnp.broadcast_to(names[i], (PACK, width)).astype(jnp.int16)
        weight = jnp.broadcast_to(scaled, (PACK, width)).astype(jnp.bfloat16)
        out.append((column, weight))
    return out


def load_rows(column_ref, share_ref, lanes, first):
    slots = column_ref.shape[0] // PACK
    return [(column_ref[i * PACK : (i + 1) * PACK, lanes], share_ref[i * PACK : (i + 1) * PACK, lanes]) for i in range(first, slots)]


def selection(slots, base, rows):
    shape = slots[0][0].shape
    iota = lax.broadcasted_iota(jnp.int32, shape, 0)
    pieces = []
    for g in range(rows // PACK):
        here = (iota + (base + g * PACK)).astype(jnp.int16)
        piece = jnp.zeros(shape, jnp.bfloat16)
        for column, weight in reversed(slots):
            piece = jnp.where(column == here, weight, piece)
        pieces.append(piece)
    return jnp.concatenate(pieces, axis=0)


def spans(total, width):
    return [pl.ds(start, min(width, total - start)) for start in range(0, total, width)]


def by_load(count, total, work):
    few = total // 4
    if few % TILE:
        return work(total)
    pl.when(count <= few)(functools.partial(work, few))
    pl.when(count > few)(functools.partial(work, total))


def gather_kernel(width, early, count_ref, index_ref, weight_ref, flipped_ref, ein_ref, column_ref, share_ref, table_ref, turned_ref):
    owned, columns = flipped_ref.shape[1], table_ref.shape[0]

    def work(total):
        for lanes in spans(total, width):
            slots = slot_rows(index_ref, weight_ref, count_ref[0], lanes)
            for i, (column, share) in enumerate(slots):
                column_ref[i * PACK : (i + 1) * PACK, lanes] = column
                share_ref[i * PACK : (i + 1) * PACK, lanes] = share
            ein_ref[:, lanes] = sum(matmul(flipped_ref[:, rows], selection(slots, rows.start, rows.size)) for rows in spans(owned, TILE))
            if lanes.start < early:
                for rows in spans(columns, TILE):
                    table = selection(slots[1:], owned + rows.start, rows.size)
                    table_ref[rows, lanes] = table
                    turned_ref[lanes, rows] = table.T

    by_load(count_ref[0], ein_ref.shape[1], work)


def element_kernel(
    width, early, pairs, owned, count_ref, visc_ref, ein_ref, column_ref, share_ref, table_ref, turned_ref, mats_v_ref, mats_p_ref, *rest
):
    n = len(pairs)
    ghost_refs, out_ref, ret_refs, rest = rest[: n + 1], rest[n + 1], rest[n + 2 : 2 * n + 2], rest[2 * n + 2 :]
    ghost_all, stacked_ref, late_ref, back = rest
    ghost, channels = ghost_refs[0].shape
    columns = table_ref.shape[0]
    spots = []
    for (distance, parity), arrived in zip(pairs, received(pairs, ghost_refs)):
        sent, _ = send_region(distance, parity)
        got = 4 * (distance - 1) + 1 - sent
        spot = pl.ds(pl.multiple_of(got * ghost, PACK), ghost)
        spots.append(spot)
        ghost_all[spot, :] = arrived

    def work(total):
        flipped = transposed(ghost_all[...])
        both = jnp.concatenate([mats_v_ref[...].T, mats_p_ref[...].T], axis=1)
        blocks = spans(total, width)
        for lanes in blocks:
            ein = ein_ref[:, lanes]
            if lanes.start < early:
                ein = ein + matmul(flipped, table_ref[:, lanes])
            else:
                slots = load_rows(column_ref, share_ref, lanes, 1)
                for rows in spans(columns, TILE):
                    table = selection(slots, owned + rows.start, rows.size)
                    late_ref[pl.ds(lanes.start - early, width), rows] = table.T
                    ein = ein + matmul(flipped[:, rows.start : rows.start + rows.size], table)
            stacked_ref[:channels, lanes] = (ein * visc_ref[:, lanes]).astype(jnp.bfloat16)
            stacked_ref[channels:, lanes] = ein.astype(jnp.bfloat16)
        for lanes in blocks:
            out_ref[:, lanes] = matmul(both, stacked_ref[:, lanes]).astype(jnp.bfloat16)
        first = min(early, total)
        summed = matmul(out_ref[:, :first], turned_ref[:first, :])
        if total > early:
            summed = summed + matmul(out_ref[:, early:total], late_ref[: total - early, :])
        back[...] = transposed(summed)
        for spot, ret_ref in zip(spots, ret_refs):
            ret_ref[...] = back[spot, :]

    by_load(count_ref[0], ein_ref.shape[1], work)


def scatter_kernel(width, count_ref, column_ref, share_ref, out_ref, names_ref, part_ref, *rest):
    hit_refs, turned_ref = rest[:-1], rest[-1]
    owned = part_ref.shape[0]

    def work(total):
        for lanes in spans(total, width):
            slots = load_rows(column_ref, share_ref, lanes, 0)
            for rows in spans(owned, TILE):
                turned_ref[lanes, rows] = selection(slots, rows.start, rows.size).T
        part_ref[...] = matmul(out_ref[:, :total], turned_ref[:total, :]).T

    by_load(count_ref[0], out_ref.shape[1], work)
    for m, hit_ref in enumerate(hit_refs):
        hit_ref[...] = one_hot(names_ref[pl.ds(m, 1), :], owned)


def finish_kernel(pairs, part_ref, *rest):
    n = len(pairs)
    hit_refs, back_refs, res_ref = rest[:n], rest[n : 2 * n + 1], rest[2 * n + 1]
    total = part_ref[...]
    for hit_ref, arrived in zip(hit_refs, received(pairs, back_refs)):
        total = total + matmul(hit_ref[...], arrived)
    res_ref[...] = total


def params(limit):
    return pltpu.CompilerParams(vmem_limit_bytes=limit * 1024 * 1024)


def cost(flops):
    return pl.CostEstimate(flops=flops, bytes_accessed=1 << 20, transcendentals=0)


def like(*arrays):
    return [jax.ShapeDtypeStruct(a.shape, a.dtype) for a in arrays]


def per_device(
    solution,
    viscosity,
    slot_index,
    slot_weight,
    mirror_rows,
    ghost_live,
    cell_count,
    viscous_block,
    pressure_block,
):
    owned, channels = solution.shape
    regions, ghost = mirror_rows.shape[1:]
    elements = viscosity.shape[0]
    width = min(TILE, elements)
    early = elements // 2
    slots = slot_index.shape[1]
    pairs = matchings(regions)
    bf16, f32 = jnp.bfloat16, jnp.float32
    table_flops = 2 * elements * channels
    list_shape = [jax.ShapeDtypeStruct((ghost, channels), bf16)] * regions
    loads = [slot_index.T, slot_weight.T, viscosity.reshape(1, elements), viscous_block, pressure_block]

    outs = pl.pallas_call(
        functools.partial(select_kernel, pairs, len(loads)),
        out_shape=list_shape
        + [
            jax.ShapeDtypeStruct((regions, ghost), jnp.int32),
            jax.ShapeDtypeStruct((channels, owned), bf16),
        ]
        + like(*loads),
        in_specs=[HBM] * (3 + len(loads)),
        out_specs=[VMEM] * (regions + 2 + len(loads)),
        scratch_shapes=[
            pltpu.VMEM(mirror_rows.shape, jnp.int32),
            pltpu.SMEM(ghost_live.shape, jnp.int32),
            pltpu.VMEM(solution.shape, bf16),
            pltpu.SemaphoreType.DMA((3 + len(loads),)),
        ],
        compiler_params=params(16),
        cost_estimate=cost(2 * owned * channels * regions * ghost),
        name="select",
    )(*[pltpu.with_memory_space_constraint(a, pltpu.HBM) for a in (mirror_rows, ghost_live, solution, *loads)])
    sent, (names, flipped, index, weight, visc, mats_v, mats_p) = outs[:regions], outs[regions:]
    got = exchange(sent, pairs)

    ein, column, share, table, turned = pl.pallas_call(
        functools.partial(gather_kernel, width, early),
        out_shape=[
            jax.ShapeDtypeStruct((channels, elements), f32),
            jax.ShapeDtypeStruct((PACK * slots, elements), jnp.int16),
            jax.ShapeDtypeStruct((PACK * slots, elements), bf16),
            jax.ShapeDtypeStruct((regions * ghost, early), bf16),
            jax.ShapeDtypeStruct((early, regions * ghost), bf16),
        ],
        in_specs=[SMEM] + [VMEM] * 3,
        out_specs=[VMEM] * 5,
        compiler_params=params(20),
        cost_estimate=cost(table_flops * owned * 8),
        name="gather_owned",
    )(cell_count, index, weight, flipped)

    out, *ret = pl.pallas_call(
        functools.partial(element_kernel, width, early, pairs, owned),
        out_shape=[jax.ShapeDtypeStruct((channels, elements), bf16)] + list_shape,
        in_specs=[SMEM] + [VMEM] * (9 + regions),
        out_specs=[VMEM] * (1 + regions),
        scratch_shapes=[
            pltpu.VMEM((regions * ghost, channels), bf16),
            pltpu.VMEM((2 * channels, elements), bf16),
            pltpu.VMEM((max(elements - early, PACK), regions * ghost), bf16),
            pltpu.VMEM((regions * ghost, channels), bf16),
        ],
        compiler_params=params(24),
        cost_estimate=cost(table_flops * regions * ghost * 2),
        name="elements",
    )(cell_count, visc, ein, column, share, table, turned, mats_v, mats_p, *got)
    back = exchange(ret, pairs)

    part, *hits = pl.pallas_call(
        functools.partial(scatter_kernel, width),
        out_shape=[jax.ShapeDtypeStruct((owned, channels), f32)] + [jax.ShapeDtypeStruct((owned, ghost), bf16)] * regions,
        in_specs=[SMEM] + [VMEM] * 4,
        out_specs=[VMEM] * (1 + regions),
        scratch_shapes=[pltpu.VMEM((elements, owned), bf16)],
        compiler_params=params(24),
        cost_estimate=cost(table_flops * owned * 8),
        name="scatter_owned",
    )(cell_count, column, share, out, names)

    return pl.pallas_call(
        functools.partial(finish_kernel, pairs),
        out_shape=jax.ShapeDtypeStruct((owned, channels), f32),
        in_specs=[VMEM] * (2 + 2 * regions),
        out_specs=VMEM,
        compiler_params=params(16),
        cost_estimate=cost(2 * owned * channels * regions * ghost),
        name="finish",
    )(part, *hits, *back)


def solution(mesh):
    return jax.shard_map(
        per_device,
        mesh=mesh,
        in_specs=(
            P(AXES, None),
            P(AXES),
            P(AXES, None),
            P(AXES, None),
            P(AXES, None, None),
            P(AXES, None),
            P(AXES),
            P(),
            P(),
        ),
        out_specs=P(AXES, None),
        check_vma=False,
    )
```
